32 devices in a mesh: wide: 16 (over z, x, core), narrow: 2 (over y).
Axes of the slice: x: 2, y: 2, z: 4, core: 2. Of those that a mesh axis runs over, the one named last changes fastest.
Arguments:
- coords: float32 [3, 16, 2048], P(None, 'narrow', 'wide'), may hold values from -1 to 1
- member: int32 [16, 2048], P('narrow', 'wide'), may hold values 0 or 1
- start_vector: float32 [3, 16, 2048], P(None, 'narrow', 'wide'), may hold values from -6 to 6
- self_block: float32 [3, 3, 16, 2048], P(None, None, 'narrow', 'wide'), may hold values from -3 to 141
- neighbour_block: float32 [6, 3, 3, 16, 2048], P(None, None, None, 'narrow', 'wide'), may hold values from -3 to 3
- neighbours: int32 [6, 16, 2048], P(None, 'narrow', 'wide'), may hold values from 0 to 7, as said below
- coarse_map: int32 [512], replicated, may hold values from 0 to 511, each once
Outputs:
- smoothed: float32 [7, 6, 3, 16, 2048], P(None, None, None, 'narrow', 'wide')
- probe_vector: float32 [3, 16, 2048], P(None, 'narrow', 'wide')
- coarse_basis: float32 [36, 512], P(None, ('wide', 'narrow'))
The draws below stay inside these ranges and needn't reach their ends.
Inputs may be any that keep to these rules, and one draw needn't show every extreme that they name: `neighbours`: the 6 codes of each node are different. `coarse_map`: each aggregate number appears once.
All inputs are finite; a program needn't handle non-finite values. No bound on the sum of `member` on one device may be relied on, other than what follows from the above.
Results may differ from the reference program's by a relative error of at most 0.0003.
Values sent between devices are 32-bit elements; how exact they have to be, the bound alone decides.
A program may use at most 64 MiB of HBM per device.

```python
import math
import jax
import jax.numpy as jnp
from jax import lax

TILE = 8
NEIGH = 6
ITERS = 4
NODES_Y = 16
NODES_X = 2048
AGGREGATES = 512


def neighbour_draw(key):
    shape = (8, NODES_Y, NODES_X)
    scores = jax.random.randint(jax.random.fold_in(key, 11), shape, 0, 2 ** 20)
    ranked = scores * 8 + lax.broadcasted_iota(jnp.int32, shape, 0)
    ranking = jnp.argsort(ranked, axis=0, stable=True)
    return ranking[:NEIGH].astype(jnp.int32)


def operator_draw(key):
    chosen = neighbour_draw(key)
    spread = max(NODES_X - 1, 1)
    col_pos = lax.broadcasted_iota(jnp.float32, (NODES_Y, NODES_X), 1)
    stiffness = 1.0 + 2.0 * col_pos / spread
    shifted = chosen + (chosen >= 4).astype(jnp.int32)
    step_x = shifted % 3 - 1
    other_col = jnp.clip(lax.broadcasted_iota(jnp.int32, chosen.shape, 2) + step_x, 0, NODES_X - 1)
    other_stiff = 1.0 + 2.0 * other_col.astype(jnp.float32) / spread
    coupling = jnp.sqrt(stiffness[None] * other_stiff)
    neighbour_part = jax.random.uniform(jax.random.fold_in(key, 12), (NEIGH, 3, 3, NODES_Y, NODES_X), jnp.float32, -1.0, 1.0)
    neighbour_part = neighbour_part * coupling[:, None, None]
    self_off = jax.random.uniform(jax.random.fold_in(key, 13), (3, 3, NODES_Y, NODES_X), jnp.float32, -1.0, 1.0)
    extra = jnp.exp(jax.random.uniform(jax.random.fold_in(key, 14), (3, NODES_Y, NODES_X), jnp.float32, 0.0, math.log(24.0)))
    identity = jnp.eye(3, dtype=jnp.float32)[:, :, None, None]
    self_part = self_off * (1.0 - identity) + identity * (23.0 + extra)[:, None]
    self_part = self_part * stiffness[None, None]
    return (self_part, neighbour_part)


def draw_self_block(key, part):
    return operator_draw(key)[0]


def draw_neighbour_block(key, part):
    return operator_draw(key)[1]


def draw_neighbours(key, part):
    return neighbour_draw(key)


def plant(values, key, low, largest):
    place = [jax.random.randint(jax.random.fold_in(key, axis), (), 0, length) for axis, length in enumerate(values.shape)]
    main_axis = values.shape.index(max(values.shape))
    beside = place[:main_axis] + [(place[main_axis] + 1) % values.shape[main_axis]] + place[main_axis + 1:]
    return values.at[tuple(place)].set(low).at[tuple(beside)].set(largest)


def block_scale(rng, dims, split, smallest, largest):
    factor_of = 1.0
    for dim, shards_of in split:
        heights = jax.random.uniform(jax.random.fold_in(jax.random.fold_in(rng, 6), dim), (shards_of,), jnp.float32, smallest / len(split), largest / len(split))
        factor_of = factor_of * jnp.repeat(jnp.exp(heights), dims[dim] // shards_of).reshape((-1,) + (1,) * (len(dims) - 1 - dim))
    return factor_of


def bell_draw(key, shape, scale, most, cuts=(), kind=jnp.bfloat16):
    loudness = block_scale(key, shape, cuts, -0.22, 0.18) if cuts else 1.0
    values = jax.random.normal(key, shape, jnp.float32) * scale * loudness
    return jnp.minimum(jnp.maximum(values, -most), most).astype(kind)


def setup_inputs(seed: int = 0) -> dict:
    keys = jax.random.split(jax.random.key(seed), 8)
    coords = jnp.clip(jax.random.uniform(keys[0], (3, NODES_Y, NODES_X), jnp.float32, -1.0, 1.0) * block_scale(keys[0], (3, NODES_Y, NODES_X), ((1, 2), (2, 16)), -0.4, 0.0), -1.0, 1.0)
    member = plant((jax.random.randint(keys[1], (NODES_Y, NODES_X), 0, 4) < 3).astype(jnp.int32), jax.random.fold_in(keys[1], 1), 0, 1)
    start_vector = bell_draw(keys[2], (3, NODES_Y, NODES_X), 1.0, 6.0, ((1, 2), (2, 16)), jnp.float32)
    self_block = draw_self_block(jax.random.fold_in(keys[7], 71), 0)
    neighbour_block = draw_neighbour_block(jax.random.fold_in(keys[7], 71), 0)
    neighbours = draw_neighbours(jax.random.fold_in(keys[7], 71), 0)
    coarse_map = jax.random.permutation(keys[6], AGGREGATES).astype(jnp.int32)
    return {"coords": coords, "member": member, "start_vector": start_vector, "self_block": self_block, "neighbour_block": neighbour_block, "neighbours": neighbours, "coarse_map": coarse_map}


def edge_index(neighbours):
    edge_count, row_count, col_count = neighbours.shape
    shifted = neighbours + (neighbours >= 4).astype(jnp.int32)
    step_y = shifted // 3 - 1
    step_x = shifted % 3 - 1
    row_pos = lax.broadcasted_iota(jnp.int32, neighbours.shape, 1)
    col_pos = lax.broadcasted_iota(jnp.int32, neighbours.shape, 2)
    linear = (row_pos + 1 + step_y) * (col_count + 2) + (col_pos + 1 + step_x)
    return linear.reshape(edge_count, row_count * col_count).astype(jnp.int32)

def edge_pieces(extended, self_block, neighbour_block, lookup):
    mode_count, comp_count = (extended.shape[0], extended.shape[1])
    row_count, col_count = (self_block.shape[2], self_block.shape[3])
    centre = extended[:, :, 1:-1, 1:-1]
    flattened = extended.reshape(mode_count, comp_count, -1)
    pieces = [jnp.sum(self_block[None] * centre[:, None], axis=2)]
    for edge_id in range(lookup.shape[0]):
        picked = jnp.take(flattened, lookup[edge_id], axis=2).reshape(mode_count, comp_count, row_count, col_count)
        pieces.append(jnp.sum(neighbour_block[edge_id][None] * picked[:, None], axis=2))
    return pieces

def summed(pieces):
    result = pieces[0]
    for addend in pieces[1:]:
        result = result + addend
    return result

def build_tentative(coords, member):
    present = member.astype(jnp.float32)
    coord_x = coords[0] * present
    coord_y = coords[1] * present
    coord_z = coords[2] * present
    blanks = jnp.zeros_like(present)
    mode_basis = jnp.stack([jnp.stack([present, blanks, blanks]), jnp.stack([blanks, present, blanks]), jnp.stack([blanks, blanks, present]), jnp.stack([-coord_y, coord_x, blanks]), jnp.stack([blanks, -coord_z, coord_y]), jnp.stack([coord_z, blanks, -coord_x])])
    row_count, col_count = present.shape
    tiles_y, tiles_x = (row_count // TILE, col_count // TILE)
    tiled = mode_basis.reshape(6, 3, tiles_y, TILE, tiles_x, TILE)
    blocks = jnp.transpose(tiled, (2, 4, 0, 1, 3, 5)).reshape(tiles_y, tiles_x, 6, 3 * TILE * TILE)
    gram_matrix = jnp.einsum('yxmr,yxnr->yxmn', blocks, blocks, precision=lax.Precision.HIGHEST)
    factor_low = jnp.linalg.cholesky(gram_matrix)
    orthonormal = jax.scipy.linalg.solve_triangular(factor_low, blocks, lower=True)
    reshaped = orthonormal.reshape(tiles_y, tiles_x, 6, 3, TILE, TILE)
    tentative = jnp.transpose(reshaped, (2, 3, 0, 4, 1, 5)).reshape(6, 3, row_count, col_count)
    return (tentative, factor_low)

def padded(values):
    return jnp.pad(values, ((0, 0), (0, 0), (1, 1), (1, 1)))

def reference(coords, member, start_vector, self_block, neighbour_block, neighbours, coarse_map):
    lookup = edge_index(neighbours)
    diagonal = jnp.stack([self_block[0, 0], self_block[1, 1], self_block[2, 2]])
    tentative, factor_low = build_tentative(coords, member)
    iterate = start_vector[None]
    curvature = jnp.float32(1.0)
    energy = jnp.float32(1.0)
    for number in range(ITERS):
        applied = summed(edge_pieces(padded(iterate), self_block, neighbour_block, lookup))
        curvature = jnp.sum(iterate * applied)
        energy = jnp.sum(iterate * diagonal * iterate)
        iterate = energy / curvature * applied / diagonal
    jacobi_weight = 4.0 * energy / (3.0 * curvature)
    pieces = edge_pieces(padded(tentative), self_block, neighbour_block, lookup)
    weighting = jacobi_weight / diagonal
    smoothed = jnp.stack([tentative - weighting * pieces[0]] + [-weighting * portion for portion in pieces[1:]])
    factor_up = jnp.swapaxes(factor_low, 2, 3).reshape(-1, 36)
    coarse_basis = jnp.take(factor_up.T, coarse_map, axis=1)
    return (smoothed, iterate[0], coarse_basis)
```

```python
import functools

import jax
import jax.numpy as jnp
from jax import lax
from jax.experimental import pallas as pl
from jax.experimental.pallas import tpu as pltpu
from jax.sharding import PartitionSpec as P

TILE = 8
ITERS = 4
MESH = pl.DeviceIdType.MESH
F32 = jnp.float32
SUMS = 10
FIELDS = 9
START, SELF, NB = 0, 3, 12
STEPS = [(-1, -1), (-1, 0), (-1, 1), (0, -1), (0, 1), (1, -1), (1, 0), (1, 1)]
VMEM_LIMIT = 16 * 1024 * 1024


def roll(x, shift, axis):
    size = x.shape[axis]
    shift = shift % size
    return x if shift == 0 else pltpu.roll(x, shift, axis)


def plane_width(wide):
    best = max(size for size in range(1, wide + 1) if wide % size == 0 and size * size <= wide)
    return wide if best == 1 else best


def edge_slots(planes, width):
    slots, tile, at = [], 0, 0
    for p in range(planes):
        columns = ITERS if p < SELF else ITERS - 1
        if at + columns > width:
            tile, at = tile + 1, 0
        slots.append((tile, at, columns))
        at += columns
    return slots, tile + 1


def kernel(
    wide, narrow, share,
    coords_h, member_h, start_h, self_h, nb_h, nbr_h, cmap_h,
    out_ref, fields, iter_ref, scale_ref, coarse_ref,
    coords, member, nbr, cmap,
    ext, wpack, stencil, pack, tedges, disp, mine, gath, sumrow, allsum, partial,
    wrecv, htrecv, vtrecv, ctrecv,
    in_sem, send_sem, recv_sem, tsend_sem, trecv_sem, gsend_sem, grecv_sem, ssend_sem, srecv_sem, far_sem,
):
    count = wide * narrow
    me_w, me_n = lax.axis_index("wide"), lax.axis_index("narrow")
    me = me_w * narrow + me_n
    barrier = pltpu.get_barrier_semaphore()
    across_plane = plane_width(wide)
    plane_count = wide // across_plane
    me_p, me_q = me_w // across_plane, lax.rem(me_w, across_plane)

    height, width = shape = member.shape
    edge_count = nbr.shape[0]
    codes_at = NB + 9 * edge_count
    planes = codes_at + edge_count
    slots, tiles = edge_slots(planes, width)
    right, left = 0, 1

    def exists(code):
        dy, dx = STEPS[code]
        ok = None
        for step, at, size in ((dy, me_n, narrow), (dx, me_w, wide)):
            term = at > 0 if step < 0 else (at < size - 1 if step > 0 else None)
            if term is not None:
                ok = term if ok is None else jnp.logical_and(ok, term)
        return ok

    present_at = [exists(code) for code in range(8)]

    def target(code):
        dy, dx = STEPS[code]
        return (me_w + dx, me_n + dy)

    def greet(cond, device):
        @pl.when(cond)
        def _():
            pl.semaphore_signal(barrier, inc=1, device_id=device, device_id_type=MESH)
        return cond.astype(jnp.int32)

    expected = 0
    for code in (1, 6, 0, 2, 5, 7, 3, 4):
        expected = expected + greet(present_at[code], target(code))

    def own(first, size):
        return ext.at[first : first + size, 0:height, 0:width]

    loads = [
        pltpu.make_async_copy(src, dst, in_sem.at[i])
        for i, (src, dst) in enumerate(
            (
                (nbr_h, nbr), (start_h, own(START, 3)), (self_h, own(SELF, 9)), (nb_h, own(NB, nb_h.shape[0])),
                (coords_h, coords), (member_h, member), (cmap_h, cmap),
            )
        )
    ]
    for load in loads:
        load.start()

    def near(w, n):
        return jnp.logical_and(jnp.abs(w - me_w) <= 1, jnp.abs(n - me_n) <= 1)

    for q in range(across_plane):
        for n in range(narrow):
            w = me_p * across_plane + q
            expected = expected + greet(jnp.logical_not(near(w, n)), (w, n))
    for p in range(plane_count):
        w = p * across_plane + me_q
        expected = expected + greet(jnp.logical_and(p != me_p, jnp.logical_not(near(w, me_n))), (w, me_n))

    for code in range(8):
        dy, dx = STEPS[code]
        @pl.when(jnp.logical_not(present_at[code]))
        def _(code=code, dy=dy, dx=dx):
            side = right if dx > 0 else left
            if dx == 0:
                at = height if dy > 0 else height + ITERS
                ext[:, at : at + ITERS, 0:width] = jnp.zeros((planes, ITERS, width), F32)
                vtrecv[0 if dy < 0 else 1] = jnp.zeros(vtrecv.shape[1:], F32)
            elif dy == 0:
                wrecv[side] = jnp.zeros(wrecv.shape[1:], F32)
                htrecv[side] = jnp.zeros(htrecv.shape[1:], F32)
            else:
                at = 0 if dy > 0 else ITERS
                wrecv[2 + side, :, at : at + ITERS, :] = jnp.zeros((tiles, ITERS, width), F32)
                ctrecv[2 * side + (0 if dy < 0 else 1)] = jnp.zeros(ctrecv.shape[1:], F32)

    lane = lax.broadcasted_iota(jnp.int32, shape, 1)
    row = lax.broadcasted_iota(jnp.int32, shape, 0)

    for load in loads[:4]:
        load.wait()
    for k in range(edge_count):
        ext[codes_at + k, 0:height, 0:width] = nbr[k].astype(F32)
    for side in (right, left):
        packed = [jnp.zeros(shape, F32) for _ in range(tiles)]
        for p, (t, at, columns) in enumerate(slots):
            first = 0 if side == left else width - columns
            moved = roll(ext[p, 0:height, 0:width], at - first, 1)
            packed[t] = moved if at == 0 else jnp.where(lane >= at, moved, packed[t])
        for t in range(tiles):
            wpack[side, t] = packed[t]

    pl.semaphore_wait(barrier, expected)

    pieces_of = {}
    for code in range(8):
        dy, dx = STEPS[code]
        if dx == 0:
            pairs = []
            for first, size, deep in ((START, 3, ITERS), (SELF, planes - SELF, ITERS - 1)):
                here = 0 if dy < 0 else height - deep
                there = height if dy < 0 else height + 2 * ITERS - deep
                pairs.append((
                    ext.at[first : first + size, here : here + deep, 0:width],
                    ext.at[first : first + size, there : there + deep, 0:width],
                ))
        else:
            mine_side, their_side = (left, right) if dx < 0 else (right, left)
            if dy == 0:
                pairs = [(wpack.at[mine_side], wrecv.at[their_side])]
            else:
                at = 0 if dy < 0 else ITERS
                pairs = [(
                    wpack.at[mine_side, :, at : at + ITERS, :], wrecv.at[2 + their_side, :, at : at + ITERS, :],
                )]
        pieces_of[code] = pairs

    copies = {}
    for code in (1, 6, 0, 2, 5, 7, 3, 4):
        made = [
            pltpu.make_async_remote_copy(
                src_ref=src, dst_ref=dst, send_sem=send_sem.at[code, i], recv_sem=recv_sem.at[7 - code, i],
                device_id=target(code), device_id_type=MESH,
            )
            for i, (src, dst) in enumerate(pieces_of[code])
        ]

        @pl.when(present_at[code])
        def _(made=made):
            for copy in made:
                copy.start()
        copies[code] = made

    for p in range(plane_count):
        @pl.when(p != me_p)
        def _(p=p):
            pl.semaphore_signal(
                far_sem, inc=1, device_id=(p * across_plane + me_q, me_n), device_id_type=MESH,
            )

    for load in loads[4:]:
        load.wait()
    present = member[...].astype(F32)
    x, y, z = (coords[r] * present for r in range(3))
    products = [present * present, x * present, y * present, z * present, x * x, y * y, z * z, x * y, x * z, y * z]
    sum_tiles = []
    for base in (0, 8):
        tile = jnp.zeros(shape, F32)
        for q, product in enumerate(products[base : base + 8]):
            tile = jnp.where(row == q, jnp.sum(product, axis=0, keepdims=True), tile)
        for s in (1, 2, 4):
            tile = tile + jnp.where((lane & s) != 0, roll(tile, s, 1), roll(tile, -s, 1))
        sum_tiles.append(tile)
    sums = [sum_tiles[q // 8][q % 8 : q % 8 + 1, :] for q in range(SUMS)]

    def factor(sums):
        n, sx, sy, sz, xx, yy, zz, xy, xz, yz = sums
        l00 = jnp.sqrt(n)
        mx, my, mz = sx / l00, sy / l00, sz / l00
        l33 = jnp.sqrt(xx + yy - mx * mx - my * my)
        l43 = (mx * mz - xz) / l33
        l53 = (my * mz - yz) / l33
        l44 = jnp.sqrt(yy + zz - my * my - mz * mz - l43 * l43)
        l54 = (mx * my - xy - l53 * l43) / l44
        l55 = jnp.sqrt(xx + zz - mx * mx - mz * mz - l53 * l53 - l54 * l54)
        return l00, mx, my, mz, l33, l43, l53, l44, l54, l55

    parts = factor(sums)
    l00, mx, my, mz, l33, l43, l53, l44, l54, l55 = parts
    unit = present / l00
    cx, cy, cz = x - mx * unit, y - my * unit, z - mz * unit
    a0, a1 = -cy / l33, cx / l33
    b0, b1, b2 = -l43 * a0 / l44, (-cz - l43 * a1) / l44, cy / l44
    g0 = (cz - l53 * a0 - l54 * b0) / l55
    g1 = (-l53 * a1 - l54 * b1) / l55
    g2 = (-cx - l54 * b2) / l55
    tent = [unit, a0, a1, b0, b1, b2, g0, g1, g2]
    packl, packr = jnp.zeros(shape, F32), jnp.zeros(shape, F32)
    for j, field in enumerate(tent):
        fields[j] = field
        packl = jnp.where(lane == j, roll(field, j, 1), packl)
        packr = jnp.where(lane == j, roll(field, j + 1, 1), packr)
        tedges[0, j : j + 1, :] = field[:1]
        tedges[1, j : j + 1, :] = field[height - 1 :]
    pack[left] = packl
    pack[right] = packr
    lane_row = lax.broadcasted_iota(jnp.int32, (1, width), 1) % 8
    rows_out = []
    for base in (0, 8):
        line = jnp.zeros((1, width), F32)
        for q, part in enumerate(parts[base : base + 8]):
            line = jnp.where(lane_row == q, part, line)
        rows_out.append(line)
    mine[0:1] = rows_out[0]
    mine[1:2] = rows_out[1]
    gath[me] = jnp.concatenate(rows_out, axis=0)

    def wait_for(code, refs, sem_of):
        @pl.when(present_at[code])
        def _():
            for i, ref in enumerate(refs):
                pltpu.make_async_copy(ref, ref, sem_of(i)).wait()

    tcopies, tarrive = {}, {}
    for code in range(8):
        dy, dx = STEPS[code]
        mine_side, their_side = (left, right) if dx < 0 else (right, left)
        if dx == 0:
            src, dst = tedges.at[0 if dy < 0 else 1], vtrecv.at[1 if dy < 0 else 0]
            arrive = vtrecv.at[0 if dy < 0 else 1]
        elif dy == 0:
            src, dst = pack.at[mine_side], htrecv.at[their_side]
            arrive = htrecv.at[mine_side]
        else:
            edge = 0 if dy < 0 else height - 1
            src = pack.at[mine_side, edge : edge + 1, :]
            dst = ctrecv.at[2 * their_side + (1 if dy < 0 else 0)]
            arrive = ctrecv.at[2 * mine_side + (0 if dy < 0 else 1)]
        copy = pltpu.make_async_remote_copy(
            src_ref=src, dst_ref=dst, send_sem=tsend_sem.at[code], recv_sem=trecv_sem.at[7 - code],
            device_id=target(code), device_id_type=MESH,
        )
        pl.when(present_at[code])(copy.start)
        tcopies[code], tarrive[code] = copy, arrive

    def by_displacement(r0, c0):
        def at(p):
            return ext[p, r0 : r0 + height, c0 : c0 + width]

        for code in range(8):
            masks = [at(codes_at + k) == code for k in range(edge_count)]
            for q in range(9):
                value = jnp.zeros(shape, F32)
                for k in range(edge_count):
                    value = jnp.where(masks[k], at(NB + 9 * k + q), value)
                stencil[code, q, r0 : r0 + height, c0 : c0 + width] = value

    by_displacement(0, 0)

    for code in (3, 4, 0, 2, 5, 7):
        dy, dx = STEPS[code]
        side = right if dx > 0 else left
        ref = wrecv.at[side]
        if dy != 0:
            at = 0 if dy > 0 else ITERS
            ref = wrecv.at[2 + side, :, at : at + ITERS, :]
        wait_for(code, [ref], lambda i, code=code: recv_sem.at[code, i])
    for part, r0 in ((0, 0), (2, height)):
        for p, (t, at, columns) in enumerate(slots):
            from_right = roll(wrecv[part + right, t], -at, 1)
            from_left = roll(wrecv[part + left, t], -at - columns, 1)
            ext[p, r0 : r0 + height, width:] = jnp.where(lane < width // 2, from_right, from_left)
    by_displacement(0, width)
    by_displacement(height, width)

    pl.semaphore_wait(far_sem, plane_count - 1)

    def to_all(src, dst, send, recv):
        def one(i):
            k, n = i // narrow, lax.rem(i, narrow)
            w = jnp.where(2 * me_w < wide, wide - 1 - k, k)
            n = lax.rem(me_n + 1 + n, narrow)

            @pl.when(jnp.logical_or(w != me_w, n != me_n))
            def _():
                pltpu.make_async_remote_copy(
                    src_ref=src, dst_ref=dst, send_sem=send, recv_sem=recv,
                    device_id=(w, n), device_id_type=MESH,
                ).start()

        pl.loop(0, count)(one)

    to_all(mine, gath.at[me], gsend_sem, grecv_sem)

    for code in (1, 6):
        dy, dx = STEPS[code]
        refs = []
        for first, size, deep in ((START, 3, ITERS), (SELF, planes - SELF, ITERS - 1)):
            at = height if dy > 0 else height + 2 * ITERS - deep
            refs.append(ext.at[first : first + size, at : at + deep, 0:width])
        wait_for(code, refs, lambda i, code=code: recv_sem.at[code, i])
    by_displacement(height, 0)

    def full(p):
        return ext[p]

    selfb = {(r, s): (lambda r=r, s=s: ext[SELF + 3 * r + s, 0:height, 0:width]) for r in range(3) for s in range(3)}
    nb = {
        (k, r, s): (lambda k=k, r=r, s=s: ext[NB + 9 * k + 3 * r + s, 0:height, 0:width])
        for k in range(edge_count) for r in range(3) for s in range(3)
    }
    elane = lax.broadcasted_iota(jnp.int32, (2 * height, 2 * width), 1)
    erow = lax.broadcasted_iota(jnp.int32, (2 * height, 2 * width), 0)

    last_row = jnp.where(me_n < narrow - 1, height + ITERS, height)
    back_row = jnp.where(me_n > 0, height + ITERS, 2 * height)
    last_lane = jnp.where(me_w < wide - 1, width + ITERS, width)
    back_lane = jnp.where(me_w > 0, 2 * width - ITERS, 2 * width)
    inside = jnp.logical_and(
        jnp.logical_or(erow < last_row, erow >= back_row), jnp.logical_or(elane < last_lane, elane >= back_lane)
    )
    inverse = [jnp.where(inside, 1.0 / full(SELF + 4 * r), 0.0) for r in range(3)]
    diag = [selfb[r, r]() for r in range(3)]
    inv = [inverse[r][:height, :width] for r in range(3)]

    iterate = [full(START + r) for r in range(3)]
    for number in range(ITERS):
        final = number == ITERS - 1
        rs, cs = (slice(0, height), slice(0, width)) if final else (slice(None), slice(None))
        applied = [sum(ext[SELF + 3 * r + s, rs, cs] * iterate[s][rs, cs] for s in range(3)) for r in range(3)]
        for s in range(3):
            for dx in (-1, 0, 1):
                shifted = roll(iterate[s], -dx, 1)
                for dy in (-1, 0, 1):
                    if (dy, dx) == (0, 0):
                        continue
                    code = STEPS.index((dy, dx))
                    moved = roll(shifted, -dy, 0)[rs, cs]
                    for r in range(3):
                        applied[r] = applied[r] + stencil[code, 3 * r + s, rs, cs] * moved
        mine_it = [v[:height, :width] for v in iterate]
        mine_ap = [v[:height, :width] for v in applied]
        curvature = sum(mine_it[r] * mine_ap[r] for r in range(3))
        energy = sum(mine_it[r] * diag[r] * mine_it[r] for r in range(3))
        partial[number : number + 1] = jnp.sum(curvature, axis=0, keepdims=True)
        partial[number + 4 : number + 5] = jnp.sum(energy, axis=0, keepdims=True)
        iterate = [applied[r] * (inv[r] if final else inverse[r]) for r in range(3)]

    totals = jnp.sum(partial[...], axis=1, keepdims=True)
    line = jnp.sum(jnp.where(lane == row, totals, 0.0), axis=0, keepdims=True)
    sumrow[...] = line
    allsum[me] = line
    to_all(sumrow, allsum.at[me], ssend_sem, srecv_sem)

    for r in range(3):
        iter_ref[r] = iterate[r]

    for code in range(8):
        wait_for(code, [tarrive[code]], lambda i, code=code: trecv_sem.at[code])

    first, last = lane == 0, lane == width - 1
    top, bottom = row == 0, row == height - 1
    lcol, rcol = htrecv[left], htrecv[right]
    corner_l = jnp.where(bottom, ctrecv[2 * left], ctrecv[2 * left + 1])
    corner_r = jnp.where(bottom, ctrecv[2 * right], ctrecv[2 * right + 1])
    for j in range(FIELDS):
        v = tent[j]
        w = jnp.where(bottom, vtrecv[0, j : j + 1, :], vtrecv[1, j : j + 1, :])
        vl = jnp.where(first, roll(lcol, -j, 1), roll(v, 1, 1))
        vr = jnp.where(last, roll(rcol, width - 1 - j, 1), roll(v, -1, 1))
        wl = jnp.where(first, roll(corner_l, -j, 1), roll(w, 1, 1))
        wr = jnp.where(last, roll(corner_r, width - 1 - j, 1), roll(w, -1, 1))
        pairs = ((vl, wl), (v, w), (vr, wr))
        up = [roll(jnp.where(bottom, b, a), 1, 0) for a, b in pairs]
        down = [roll(jnp.where(top, b, a), -1, 0) for a, b in pairs]
        for code, moved in enumerate(up + [vl, vr] + down):
            disp[j, code] = moved

    def piece(block, picked, index):
        unit, a0, a1, b0, b1, b2, g0, g1, g2 = picked
        for r in range(3):
            c0, c1, c2 = (block(r, s) * -inv[r] for s in range(3))
            out_ref[index, 0, r] = c0 * unit
            out_ref[index, 1, r] = c1 * unit
            out_ref[index, 2, r] = c2 * unit
            out_ref[index, 3, r] = c0 * a0 + c1 * a1
            out_ref[index, 4, r] = c0 * b0 + c1 * b1 + c2 * b2
            out_ref[index, 5, r] = c0 * g0 + c1 * g1 + c2 * g2

    piece(lambda r, s: selfb[r, s](), [fields[j] for j in range(FIELDS)], 0)
    for k in range(edge_count):
        masks = [nbr[k] == code for code in range(1, 8)]
        picked = []
        for j in range(FIELDS):
            value = disp[j, 0]
            for code in range(1, 8):
                value = jnp.where(masks[code - 1], disp[j, code], value)
            picked.append(value)
        piece(lambda r, s: nb[k, r, s](), picked, k + 1)

    some = gath.at[pl.ds(0, count - 1)]
    pltpu.make_async_copy(some, some, grecv_sem).wait()
    across = width // TILE * wide
    tiles_x, tiles_y = width // TILE, height // TILE
    crow = lax.broadcasted_iota(jnp.int32, (share, width), 0)
    cgroup = lax.broadcasted_iota(jnp.int32, (share, width), 1) // TILE
    low, high = jnp.zeros((share, width), F32), jnp.zeros((share, width), F32)
    for j in range(share):
        wanted = cmap[me * share + j]
        tile_row, tile_col = wanted // across, lax.rem(wanted, across)
        slot = tile_col // tiles_x * narrow + tile_row // tiles_y
        lines = gath[slot]
        take = jnp.logical_and(crow == j, cgroup == lax.rem(tile_col, tiles_x))
        low = jnp.where(take, lines[0:1], low)
        high = jnp.where(take, lines[1:2], high)
    l00, mx, my, mz, l33, l43, l53, l44, l54, l55 = range(SUMS)
    entries = {
        (0, 0): (l00, 1), (1, 1): (l00, 1), (2, 2): (l00, 1),
        (3, 0): (my, -1), (3, 1): (mx, 1), (4, 1): (mz, -1), (4, 2): (my, 1), (5, 0): (mz, 1), (5, 2): (mx, -1),
        (3, 3): (l33, 1), (4, 3): (l43, 1), (5, 3): (l53, 1), (4, 4): (l44, 1), (5, 4): (l54, 1), (5, 5): (l55, 1),
    }
    outs = coarse_ref.shape[1]
    kind = lax.broadcasted_iota(jnp.int32, (1, outs), 1)
    chosen, sign = jnp.full((1, outs), -1, jnp.int32), jnp.zeros((1, outs), F32)
    for (n, m), (q, way) in entries.items():
        chosen = jnp.where(kind == 6 * m + n, q, chosen)
        sign = jnp.where(kind == 6 * m + n, float(way), sign)
    entry = lax.broadcasted_iota(jnp.int32, (width, outs), 0) % 8
    coarse = jnp.zeros(coarse_ref.shape, F32)
    for base, lines in ((0, low), (8, high)):
        pick = jnp.where(entry + base == chosen, sign, 0.0)
        coarse = coarse + jnp.dot(lines, pick, precision=lax.Precision.HIGHEST, preferred_element_type=F32)
    coarse_ref[...] = coarse

    for code in range(8):
        @pl.when(present_at[code])
        def _(code=code):
            for copy in copies[code] + [tcopies[code]]:
                copy.wait_send()
    for buffer, sem in ((gath, gsend_sem), (allsum, ssend_sem)):
        some = buffer.at[pl.ds(0, count - 1)]
        pltpu.make_async_copy(some, some, sem).wait()

    some = allsum.at[pl.ds(0, count - 1)]
    pltpu.make_async_copy(some, some, srecv_sem).wait()
    if count <= 64:
        lines = [allsum[d] for d in range(count)]
        while len(lines) > 1:
            lines = [a + b for a, b in zip(lines[::2], lines[1::2])] + ([lines[-1]] if len(lines) % 2 else [])
        total = lines[0]
    else:
        total = lax.fori_loop(0, count, lambda d, t: t + allsum[d], jnp.zeros((1, width), F32))
    values = [jnp.broadcast_to(total[:, i : i + 1], shape) for i in range(2 * ITERS)]
    ratios = [values[i + ITERS] / values[i] for i in range(ITERS)]
    growth = ratios[0]
    for i in range(1, ITERS):
        growth = growth * ratios[i]
    scale_ref[0] = ratios[ITERS - 1] * (4.0 / 3.0)
    scale_ref[1] = growth


def finish(raw, fields, iterate, scale, coarse, out_h, probe_h, coarse_h, out, probe, sem):
    weight = scale[0]
    base = {(0, 0): 0, (1, 1): 0, (2, 2): 0, (3, 0): 1, (3, 1): 2}
    for r in range(3):
        base[(4, r)] = 3 + r
        base[(5, r)] = 6 + r
    blocks, modes = raw.shape[:2]
    last = pltpu.make_async_copy(coarse, coarse_h, sem.at[blocks + 1])
    last.start()
    copies = [last]
    for k in range(blocks):
        for m in range(modes):
            for r in range(3):
                value = raw[k, m, r] * weight
                out[k, m, r] = value + fields[base[(m, r)]] if k == 0 and (m, r) in base else value
        copy = pltpu.make_async_copy(out.at[k], out_h.at[k], sem.at[k])
        copy.start()
        copies.append(copy)
    for r in range(3):
        probe[r] = iterate[r] * scale[1]
    copy = pltpu.make_async_copy(probe, probe_h, sem.at[blocks])
    copy.start()
    copies.append(copy)
    for copy in copies:
        copy.wait()


def local(wide, narrow, coords, member, start_vector, self_block, neighbour_block, neighbours, coarse_map):
    height, width = member.shape
    edge_count = neighbours.shape[0]
    count = wide * narrow
    share = coarse_map.shape[0] // count
    tile = (height, width)
    double = (2 * height, 2 * width)
    planes = 12 + 10 * edge_count
    tiles = edge_slots(planes, width)[1]
    vmem = pltpu.VMEM
    dma = pltpu.SemaphoreType.DMA
    results = (
        jax.ShapeDtypeStruct((edge_count + 1, 6, 3) + tile, F32),
        jax.ShapeDtypeStruct((3,) + tile, F32),
        jax.ShapeDtypeStruct((share, 36), F32),
    )
    staged = pl.pallas_call(
        functools.partial(kernel, wide, narrow, share),
        out_shape=(
            results[0],
            jax.ShapeDtypeStruct((FIELDS,) + tile, F32),
            results[1],
            jax.ShapeDtypeStruct((2,) + tile, F32),
            results[2],
        ),
        in_specs=[pl.BlockSpec(memory_space=pl.ANY)] * 7,
        out_specs=(pl.BlockSpec(memory_space=pltpu.VMEM),) * 5,
        scratch_shapes=[
            vmem((3,) + tile, F32),
            vmem(tile, jnp.int32),
            vmem((edge_count,) + tile, jnp.int32),
            pltpu.SMEM(coarse_map.shape, jnp.int32),
            vmem((planes,) + double, F32),
            vmem((2, tiles) + tile, F32),
            vmem((8, 9) + double, F32),
            vmem((2,) + tile, F32),
            vmem((2, 16, width), F32),
            vmem((FIELDS, 8) + tile, F32),
            vmem((2, width), F32),
            vmem((count, 2, width), F32),
            vmem((1, width), F32),
            vmem((count, 1, width), F32),
            vmem((8, width), F32),
            vmem((4, tiles) + tile, F32),
            vmem((2,) + tile, F32),
            vmem((2, 16, width), F32),
            vmem((4, 1, width), F32),
            dma((7,)),
            dma((8, 2)),
            dma((8, 2)),
            dma((8,)),
            dma((8,)),
            dma(()),
            dma(()),
            dma(()),
            dma(()),
            pltpu.SemaphoreType.REGULAR,
        ],
        compiler_params=pltpu.CompilerParams(collective_id=0, has_side_effects=True, vmem_limit_bytes=VMEM_LIMIT),
    )(*(
        pltpu.with_memory_space_constraint(value, pltpu.HBM)
        for value in (
            coords, member, start_vector, self_block.reshape((9,) + tile), neighbour_block.reshape((-1,) + tile),
            neighbours, coarse_map,
        )
    ))
    smoothed, probe, coarse = pl.pallas_call(
        finish,
        out_shape=results,
        in_specs=[pl.BlockSpec(memory_space=pltpu.VMEM)] * 5,
        out_specs=(pl.BlockSpec(memory_space=pl.ANY),) * 3,
        scratch_shapes=[
            vmem(results[0].shape, F32),
            vmem(results[1].shape, F32),
            dma((edge_count + 3,)),
        ],
        compiler_params=pltpu.CompilerParams(vmem_limit_bytes=VMEM_LIMIT),
    )(*staged)
    return smoothed, probe, coarse.T


def solution(mesh):
    return jax.shard_map(
        functools.partial(local, mesh.shape["wide"], mesh.shape["narrow"]),
        mesh=mesh,
        in_specs=(
            P(None, "narrow", "wide"),
            P("narrow", "wide"),
            P(None, "narrow", "wide"),
            P(None, None, "narrow", "wide"),
            P(None, None, None, "narrow", "wide"),
            P(None, "narrow", "wide"),
            P(),
        ),
        out_specs=(
            P(None, None, None, "narrow", "wide"),
            P(None, "narrow", "wide"),
            P(None, ("wide", "narrow")),
        ),
        check_vma=False,
    )
```

```python
import functools

import jax
import jax.numpy as jnp
from jax import lax
from jax.experimental import pallas as pl
from jax.experimental.pallas import tpu as pltpu
from jax.sharding import PartitionSpec as P

TILE = 8
ITERS = 4
MESH = pl.DeviceIdType.MESH
F32 = jnp.float32
SUMS = 10
FIELDS = 9
START, SELF, NB = 0, 3, 12
STEPS = [(-1, -1), (-1, 0), (-1, 1), (0, -1), (0, 1), (1, -1), (1, 0), (1, 1)]
VMEM_LIMIT = 16 * 1024 * 1024


def roll(x, shift, axis):
    size = x.shape[axis]
    shift = shift % size
    return x if shift == 0 else pltpu.roll(x, shift, axis)


def plane_width(wide):
    best = max(size for size in range(1, wide + 1) if wide % size == 0 and size * size <= wide)
    return wide if best == 1 else best


def edge_slots(planes, width):
    per = width // (ITERS - 1)
    tiles = pl.cdiv(planes - SELF, per)
    slots = [(tiles, ITERS * p, ITERS) for p in range(SELF)]
    slots += [(p // per, p % per * (ITERS - 1), ITERS - 1) for p in range(planes - SELF)]
    return slots, tiles


def rounds_of(across_plane, narrow):
    offsets, reach = [1], 1
    while reach < max(across_plane, narrow) - 1:
        offsets.append(reach + 1)
        reach = 2 * reach + 1
    return offsets


IN_ROWS, IN_COORDS, IN_MAP = range(3)
SIDES, CORNERS, STARTS, BANDS, EDGES, GATHER, TOTALS = range(7)


def kernel(
    wide, narrow, share,
    coords_h, member_h, start_h, self_h, nb_h, nbr_h, cmap_h,
    out_ref, fields, iter_ref, scale_ref, coarse_ref,
    coords, member, nbr, cmap,
    ext, wpack, stencil, pack, tedges, disp, mine, gath, sumrow, allsum, partial,
    wrecv, htrecv, vtrecv, ctrecv, firsts_own, firsts,
    tally, in_sem, send_sem, recv_sem, round_sem,
):
    count = wide * narrow
    me_w, me_n = lax.axis_index("wide"), lax.axis_index("narrow")
    me = me_w * narrow + me_n
    barrier = pltpu.get_barrier_semaphore()
    across_plane = plane_width(wide)
    plane_count = wide // across_plane
    me_p, me_q = me_w // across_plane, lax.rem(me_w, across_plane)

    height, width = shape = member.shape
    edge_count = nbr.shape[0]
    codes_at = NB + 9 * edge_count
    planes = codes_at + edge_count
    slots, tiles = edge_slots(planes, width)
    offsets = rounds_of(across_plane, narrow)
    right, left = 0, 1

    def exists(code):
        dy, dx = STEPS[code]
        ok = None
        for step, at, size in ((dy, me_n, narrow), (dx, me_w, wide)):
            term = at > 0 if step < 0 else (at < size - 1 if step > 0 else None)
            if term is not None:
                ok = term if ok is None else jnp.logical_and(ok, term)
        return ok

    present_at = [exists(code) for code in range(8)]

    def target(code):
        dy, dx = STEPS[code]
        return (me_w + dx, me_n + dy)

    def greet(cond, device):
        @pl.when(cond)
        def _():
            pl.semaphore_signal(barrier, inc=1, device_id=device, device_id_type=MESH)
        return cond.astype(jnp.int32)

    expected = 0
    for code in (1, 6):
        expected = expected + greet(present_at[code], target(code))

    def own(first, size):
        return ext.at[first : first + size, 0:height, 0:width]

    loads = [
        pltpu.make_async_copy(src, dst, in_sem.at[i])
        for src, dst, i in (
            (nb_h, own(NB, nb_h.shape[0]), IN_ROWS), (self_h, own(SELF, 9), IN_ROWS), (start_h, own(START, 3), IN_ROWS),
            (nbr_h, nbr, IN_ROWS), (coords_h, coords, IN_COORDS), (member_h, member, IN_COORDS), (cmap_h, cmap, IN_MAP),
        )
    ]
    for load in loads:
        load.start()

    def wait_rows(sem, rows):
        some = tally.at[0:rows]
        pltpu.make_async_copy(some, some, sem).wait()

    sides_here = (me_w > 0).astype(jnp.int32) + (me_w < wide - 1).astype(jnp.int32)
    ends_here = (me_n > 0).astype(jnp.int32) + (me_n < narrow - 1).astype(jnp.int32)

    def wait_halo(sem, side, end, corner, more=0):
        for a in range(min(wide - 1, 1), min(wide - 1, 2) + 1):
            for b in range(min(narrow - 1, 1), min(narrow - 1, 2) + 1):
                rows = a * side + b * end + a * b * corner + more
                if rows:
                    pl.when(jnp.logical_and(sides_here == a, ends_here == b))(functools.partial(wait_rows, sem, rows))

    for code in (0, 2, 5, 7, 3, 4):
        expected = expected + greet(present_at[code], target(code))

    for p in range(plane_count):
        w = p * across_plane + me_q
        expected = expected + greet(jnp.abs(w - me_w) > 1, (w, me_n))

    def partners(offset):
        for dq in (-offset, 0, offset):
            for dn in (-offset, 0, offset):
                if (dq, dn) != (0, 0) and abs(dq) < across_plane and abs(dn) < narrow:
                    q, n = me_q + dq, me_n + dn
                    fits = [cond for step, cond in (
                        (-dq, q >= 0), (dq, q < across_plane), (-dn, n >= 0), (dn, n < narrow),
                    ) if step > 0]
                    yield functools.reduce(jnp.logical_and, fits), (me_w + dq, n)

    def tell(number):
        for cond, device in partners(offsets[number]):
            @pl.when(cond)
            def _(device=device):
                pl.semaphore_signal(round_sem.at[number], inc=1, device_id=device, device_id_type=MESH)

    def hear(number):
        pl.semaphore_wait(round_sem.at[number], sum(cond.astype(jnp.int32) for cond, _ in partners(offsets[number])))

    deep = ITERS - 1

    def corner_refs(ref, low):
        at = 0 if low else height - deep
        start_at = 0 if low else height - ITERS
        return [ref.at[0:tiles, at : at + deep, :], ref.at[tiles, start_at : start_at + ITERS, :]]

    for code in range(8):
        dy, dx = STEPS[code]
        @pl.when(jnp.logical_not(present_at[code]))
        def _(code=code, dy=dy, dx=dx):
            side = right if dx > 0 else left
            if dx == 0:
                at = height if dy > 0 else height + ITERS
                ext[:, at : at + ITERS, 0:width] = jnp.zeros((planes, ITERS, width), F32)
                vtrecv[0 if dy < 0 else 1] = jnp.zeros(vtrecv.shape[1:], F32)
                at = deep - 1 if dy > 0 else height - deep
                firsts[:, at : at + 1, :] = jnp.zeros((3, 1, width), F32)
                at = deep if dy > 0 else height - deep - 1
                for to in (right, left):
                    wrecv[2 + to, 0:tiles, at : at + 1, :] = jnp.zeros((tiles, 1, width), F32)
            elif dy == 0:
                wrecv[side] = jnp.zeros(wrecv.shape[1:], F32)
                htrecv[side] = jnp.zeros(htrecv.shape[1:], F32)
            else:
                for ref in corner_refs(wrecv.at[2 + side], dy > 0):
                    ref[...] = jnp.zeros(ref.shape, F32)
                ctrecv[2 * side + (0 if dy < 0 else 1)] = jnp.zeros(ctrecv.shape[1:], F32)

    lane = lax.broadcasted_iota(jnp.int32, shape, 1)
    row = lax.broadcasted_iota(jnp.int32, shape, 0)
    first, last = lane == 0, lane == width - 1

    wait_rows(in_sem.at[IN_ROWS], planes * height)
    for k in range(edge_count):
        ext[codes_at + k, 0:height, 0:width] = nbr[k].astype(F32)

    pl.semaphore_wait(barrier, expected)
    tell(0)

    def send(code, pairs, group):
        made = [
            pltpu.make_async_remote_copy(
                src_ref=src, dst_ref=dst, send_sem=send_sem, recv_sem=recv_sem.at[group],
                device_id=target(code), device_id_type=MESH,
            )
            for src, dst in pairs
        ]

        @pl.when(present_at[code])
        def _():
            for copy in made:
                copy.start()

    bands = ((START, 3, ITERS), (SELF, 9, deep - 1), (NB, planes - NB, deep - 1))

    def band_pairs(code, band):
        base, size, rows = band
        here, there = (0, height) if STEPS[code][0] < 0 else (height - rows, height + 2 * ITERS - rows)
        return [(
            ext.at[base : base + size, here : here + rows, 0:width],
            ext.at[base : base + size, there : there + rows, 0:width],
        )]

    def end_pairs(code):
        here, there = (deep - 1, deep) if STEPS[code][0] < 0 else (height - deep, height - deep - 1)
        return [
            (wpack.at[side, 0:tiles, here : here + 1, :], wrecv.at[3 - side, 0:tiles, there : there + 1, :])
            for side in (right, left)
        ]

    def first_pairs(code):
        here = deep - 1 if STEPS[code][0] < 0 else height - deep
        return [(firsts_own.at[:, here : here + 1, :], firsts.at[:, here : here + 1, :])]

    for code in (1, 6):
        send(code, band_pairs(code, bands[0]), STARTS)
        send(code, band_pairs(code, bands[1]), BANDS)
    for side in (right, left):
        packed = [jnp.zeros(shape, F32) for _ in range(tiles + 1)]
        for p, (t, at, columns) in enumerate(slots):
            begin = 0 if side == left else width - columns
            moved = roll(ext[p, 0:height, 0:width], at - begin, 1)
            packed[t] = moved if at == 0 else jnp.where(lane >= at, moved, packed[t])
        for t in range(tiles + 1):
            wpack[side, t] = packed[t]

    for code in (0, 2, 5, 7, 3, 4):
        dy, dx = STEPS[code]
        mine_side, their_side = (left, right) if dx < 0 else (right, left)
        if dy == 0:
            send(code, [(wpack.at[mine_side], wrecv.at[their_side])], SIDES)
        else:
            send(code, list(zip(
                corner_refs(wpack.at[mine_side], dy < 0), corner_refs(wrecv.at[2 + their_side], dy < 0),
            )), CORNERS)
    for code in (1, 6):
        send(code, end_pairs(code), CORNERS)
        send(code, band_pairs(code, bands[2]), BANDS)

    def by_displacement(r0, c0):
        def at(p):
            return ext[p, r0 : r0 + height, c0 : c0 + width]

        for group in range(0, 8, 2):
            masks = {(code, k): at(codes_at + k) == code for code in (group, group + 1) for k in range(edge_count)}
            for q in range(9):
                blocks = [at(NB + 9 * k + q) for k in range(edge_count)]
                for code in (group, group + 1):
                    value = jnp.zeros(shape, F32)
                    for k in range(edge_count):
                        value = jnp.where(masks[code, k], blocks[k], value)
                    stencil[code, q, r0 : r0 + height, c0 : c0 + width] = value

    def apply(iterate, rs, cs):
        applied = [sum(ext[SELF + 3 * r + s, rs, cs] * iterate[s][rs, cs] for s in range(3)) for r in range(3)]
        for s in range(3):
            for dx in (0, -1, 1):
                shifted = roll(iterate[s], -dx, 1)
                for dy in (-1, 0, 1):
                    if (dy, dx) == (0, 0):
                        continue
                    code = STEPS.index((dy, dx))
                    moved = roll(shifted, -dy, 0)[rs, cs]
                    for r in range(3):
                        applied[r] = applied[r] + stencil[code, 3 * r + s, rs, cs] * moved
        return applied

    by_displacement(0, 0)
    inside_rows, inside_cols = slice(0, height), slice(0, width)
    applied = apply([ext[START + r, 0:height, 0:width] for r in range(3)], inside_rows, inside_cols)
    for r in range(3):
        firsts_own[r] = applied[r] * (1.0 / ext[SELF + 4 * r, 0:height, 0:width])
    for code in (1, 6):
        send(code, first_pairs(code), BANDS)

    wait_rows(in_sem.at[IN_COORDS], 4 * height)
    present = member[...].astype(F32)
    x, y, z = (coords[r] * present for r in range(3))
    products = [present * present, x * present, y * present, z * present, x * x, y * y, z * z, x * y, x * z, y * z]
    sum_tiles = []
    for base in (0, 8):
        tile = jnp.zeros(shape, F32)
        for q, product in enumerate(products[base : base + 8]):
            tile = jnp.where(row == q, jnp.sum(product, axis=0, keepdims=True), tile)
        for s in (1, 2, 4):
            tile = tile + jnp.where((lane & s) != 0, roll(tile, s, 1), roll(tile, -s, 1))
        sum_tiles.append(tile)
    sums = [sum_tiles[q // 8][q % 8 : q % 8 + 1, :] for q in range(SUMS)]

    def factor(sums):
        n, sx, sy, sz, xx, yy, zz, xy, xz, yz = sums
        l00 = jnp.sqrt(n)
        mx, my, mz = sx / l00, sy / l00, sz / l00
        l33 = jnp.sqrt(xx + yy - mx * mx - my * my)
        l43 = (mx * mz - xz) / l33
        l53 = (my * mz - yz) / l33
        l44 = jnp.sqrt(yy + zz - my * my - mz * mz - l43 * l43)
        l54 = (mx * my - xy - l53 * l43) / l44
        l55 = jnp.sqrt(xx + zz - mx * mx - mz * mz - l53 * l53 - l54 * l54)
        return l00, mx, my, mz, l33, l43, l53, l44, l54, l55

    parts = factor(sums)
    l00, mx, my, mz, l33, l43, l53, l44, l54, l55 = parts
    unit = present / l00
    cx, cy, cz = x - mx * unit, y - my * unit, z - mz * unit
    a0, a1 = -cy / l33, cx / l33
    b0, b1, b2 = -l43 * a0 / l44, (-cz - l43 * a1) / l44, cy / l44
    g0 = (cz - l53 * a0 - l54 * b0) / l55
    g1 = (-l53 * a1 - l54 * b1) / l55
    g2 = (-cx - l54 * b2) / l55
    tent = [unit, a0, a1, b0, b1, b2, g0, g1, g2]
    packl, packr = jnp.zeros(shape, F32), jnp.zeros(shape, F32)
    for j, field in enumerate(tent):
        fields[j] = field
        packl = jnp.where(lane == j, roll(field, j, 1), packl)
        packr = jnp.where(lane == j, roll(field, j + 1, 1), packr)
        tedges[0, j] = field[:1]
        tedges[1, j] = field[height - 1 :]
    pack[left] = packl
    pack[right] = packr
    lane_row = lax.broadcasted_iota(jnp.int32, (1, width), 1) % 8
    rows_out = []
    for base in (0, 8):
        line = jnp.zeros((1, width), F32)
        for q, part in enumerate(parts[base : base + 8]):
            line = jnp.where(lane_row == q, part, line)
        rows_out.append(line)
    mine[0:1] = rows_out[0]
    mine[1:2] = rows_out[1]
    gath[me] = jnp.concatenate(rows_out, axis=0)

    for code in range(8):
        dy, dx = STEPS[code]
        mine_side, their_side = (left, right) if dx < 0 else (right, left)
        if dx == 0:
            src, dst = tedges.at[0 if dy < 0 else 1], vtrecv.at[1 if dy < 0 else 0]
        elif dy == 0:
            src, dst = pack.at[mine_side], htrecv.at[their_side]
        else:
            edge = 0 if dy < 0 else height - 1
            src = pack.at[mine_side, edge : edge + 1, :]
            dst = ctrecv.at[2 * their_side + (1 if dy < 0 else 0)]
        send(code, [(src, dst)], EDGES)

    for number in range(len(offsets) - 1):
        hear(number)
        tell(number + 1)
    def unpack(part, r0):
        for p, (t, at, columns) in enumerate(slots):
            from_right = roll(wrecv[part + right, t], -at, 1)
            from_left = roll(wrecv[part + left, t], -at - columns, 1)
            both = jnp.where(lane < width // 2, from_right, from_left)
            ext[p, r0 : r0 + height, width:] = both
            if part and p >= SELF:
                ext[p, height + deep - 1 : height + deep, 0:width] = both[deep : deep + 1]
                ext[p, 2 * height - deep : 2 * height - deep + 1, 0:width] = both[height - deep - 1 : height - deep]

    side_rows, start_rows = (tiles + 1) * height, SELF * ITERS
    corner_rows, end_rows = tiles * deep + ITERS, 2 * tiles
    band_rows = (planes - SELF) * (deep - 1) + 3
    edge_rows = (height, FIELDS, 1)
    wait_halo(recv_sem.at[SIDES], side_rows, 0, 0)
    unpack(0, 0)
    by_displacement(0, width)

    hear(len(offsets) - 1)

    def to_all(src, dst, group):
        def one(i):
            k = i // narrow
            w = jnp.where(2 * me_w < wide, wide - 1 - k, k)
            n = lax.rem(me_n + 1 + i, narrow)

            @pl.when(jnp.logical_or(w != me_w, n != me_n))
            def _():
                pltpu.make_async_remote_copy(
                    src_ref=src, dst_ref=dst, send_sem=send_sem, recv_sem=recv_sem.at[group],
                    device_id=(w, n), device_id_type=MESH,
                ).start()

        if count <= 64:
            for i in range(count):
                one(i)
        else:
            pl.loop(0, count)(one)

    to_all(mine, gath.at[me], GATHER)

    wait_halo(recv_sem.at[CORNERS], 0, end_rows, corner_rows)
    unpack(2, height)
    by_displacement(height, width)
    wait_halo(recv_sem.at[STARTS], 0, start_rows, 0)
    whole_cols, beyond = slice(None), slice(width, None)
    begin = [ext[START + r] for r in range(3)]
    begin_top = apply(begin, inside_rows, whole_cols)
    begin_corner = apply(begin, slice(height, None), beyond)
    wait_halo(recv_sem.at[BANDS], 0, band_rows, 0)
    by_displacement(height, 0)

    def full(p):
        return ext[p]

    selfb = {(r, s): (lambda r=r, s=s: ext[SELF + 3 * r + s, 0:height, 0:width]) for r in range(3) for s in range(3)}
    nb = {
        (k, r, s): (lambda k=k, r=r, s=s: ext[NB + 9 * k + 3 * r + s, 0:height, 0:width])
        for k in range(edge_count) for r in range(3) for s in range(3)
    }
    elane = lax.broadcasted_iota(jnp.int32, (2 * height, 2 * width), 1)
    erow = lax.broadcasted_iota(jnp.int32, (2 * height, 2 * width), 0)

    last_row = jnp.where(me_n < narrow - 1, height + ITERS, height)
    back_row = jnp.where(me_n > 0, height + ITERS, 2 * height)
    last_lane = jnp.where(me_w < wide - 1, width + ITERS, width)
    back_lane = jnp.where(me_w > 0, 2 * width - ITERS, 2 * width)
    inside = jnp.logical_and(
        jnp.logical_or(erow < last_row, erow >= back_row), jnp.logical_or(elane < last_lane, elane >= back_lane)
    )
    inverse = [jnp.where(inside, 1.0 / full(SELF + 4 * r), 0.0) for r in range(3)]
    diag = [selfb[r, r]() for r in range(3)]
    inv = [inverse[r][:height, :width] for r in range(3)]

    sent = jnp.logical_and(
        jnp.logical_or(erow == height + deep - 1, erow == 2 * height - deep),
        jnp.logical_and(elane > 0, elane < width - 1),
    )
    spread = [
        jnp.concatenate([jnp.concatenate([firsts[r], firsts[r]], axis=0)] * 2, axis=1) for r in range(3)
    ]
    iterate = begin
    for number in range(ITERS):
        final = number == ITERS - 1
        rs, cs = (slice(0, height), slice(0, width)) if final else (slice(None), slice(None))
        if number == 0:
            outer = apply(begin, slice(height, None), inside_cols)
            applied = [
                jnp.concatenate([begin_top[r], jnp.concatenate([outer[r], begin_corner[r]], axis=1)], axis=0) for r in range(3)
            ]
        else:
            applied = apply(iterate, rs, cs)
        mine_it = [v[:height, :width] for v in iterate]
        mine_ap = [v[:height, :width] for v in applied]
        curvature = sum(mine_it[r] * mine_ap[r] for r in range(3))
        energy = sum(mine_it[r] * diag[r] * mine_it[r] for r in range(3))
        partial[number : number + 1] = jnp.sum(curvature, axis=0, keepdims=True)
        partial[number + 4 : number + 5] = jnp.sum(energy, axis=0, keepdims=True)
        iterate = [applied[r] * (inv[r] if final else inverse[r]) for r in range(3)]
        if number == 0:
            iterate = [jnp.where(sent, spread[r], iterate[r]) for r in range(3)]

    totals = jnp.sum(partial[...], axis=1, keepdims=True)
    line = jnp.sum(jnp.where(lane == row, totals, 0.0), axis=0, keepdims=True)
    sumrow[...] = line
    allsum[me] = line
    to_all(sumrow, allsum.at[me], TOTALS)

    for r in range(3):
        iter_ref[r] = iterate[r]

    wait_halo(recv_sem.at[EDGES], *edge_rows)

    top, bottom = row == 0, row == height - 1
    lcol, rcol = htrecv[left], htrecv[right]
    corner_l = jnp.where(bottom, ctrecv[2 * left], ctrecv[2 * left + 1])
    corner_r = jnp.where(bottom, ctrecv[2 * right], ctrecv[2 * right + 1])
    for j in range(FIELDS):
        v = tent[j]
        w = jnp.where(bottom, vtrecv[0, j], vtrecv[1, j])
        vl = jnp.where(first, roll(lcol, -j, 1), roll(v, 1, 1))
        vr = jnp.where(last, roll(rcol, width - 1 - j, 1), roll(v, -1, 1))
        wl = jnp.where(first, roll(corner_l, -j, 1), roll(w, 1, 1))
        wr = jnp.where(last, roll(corner_r, width - 1 - j, 1), roll(w, -1, 1))
        pairs = ((vl, wl), (v, w), (vr, wr))
        up = [roll(jnp.where(bottom, b, a), 1, 0) for a, b in pairs]
        down = [roll(jnp.where(top, b, a), -1, 0) for a, b in pairs]
        for code, moved in enumerate(up + [vl, vr] + down):
            disp[j, code] = moved

    def piece(block, picked, index):
        unit, a0, a1, b0, b1, b2, g0, g1, g2 = picked
        for r in range(3):
            c0, c1, c2 = (block(r, s) * -inv[r] for s in range(3))
            out_ref[index, 0, r] = c0 * unit
            out_ref[index, 1, r] = c1 * unit
            out_ref[index, 2, r] = c2 * unit
            out_ref[index, 3, r] = c0 * a0 + c1 * a1
            out_ref[index, 4, r] = c0 * b0 + c1 * b1 + c2 * b2
            out_ref[index, 5, r] = c0 * g0 + c1 * g1 + c2 * g2

    piece(lambda r, s: selfb[r, s](), [fields[j] for j in range(FIELDS)], 0)
    for k in range(edge_count):
        masks = [nbr[k] == code for code in range(1, 8)]
        picked = []
        for j in range(FIELDS):
            value = disp[j, 0]
            for code in range(1, 8):
                value = jnp.where(masks[code - 1], disp[j, code], value)
            picked.append(value)
        piece(lambda r, s: nb[k, r, s](), picked, k + 1)

    loads[6].wait()
    some = gath.at[pl.ds(0, count - 1)]
    pltpu.make_async_copy(some, some, recv_sem.at[GATHER]).wait()
    across = width // TILE * wide
    tiles_x, tiles_y = width // TILE, height // TILE
    crow = lax.broadcasted_iota(jnp.int32, (share, width), 0)
    cgroup = lax.broadcasted_iota(jnp.int32, (share, width), 1) // TILE
    low, high = jnp.zeros((share, width), F32), jnp.zeros((share, width), F32)
    for j in range(share):
        wanted = cmap[me * share + j]
        tile_row, tile_col = wanted // across, lax.rem(wanted, across)
        slot = tile_col // tiles_x * narrow + tile_row // tiles_y
        lines = gath[slot]
        take = jnp.logical_and(crow == j, cgroup == lax.rem(tile_col, tiles_x))
        low = jnp.where(take, lines[0:1], low)
        high = jnp.where(take, lines[1:2], high)
    l00, mx, my, mz, l33, l43, l53, l44, l54, l55 = range(SUMS)
    entries = {
        (0, 0): (l00, 1), (1, 1): (l00, 1), (2, 2): (l00, 1),
        (3, 0): (my, -1), (3, 1): (mx, 1), (4, 1): (mz, -1), (4, 2): (my, 1), (5, 0): (mz, 1), (5, 2): (mx, -1),
        (3, 3): (l33, 1), (4, 3): (l43, 1), (5, 3): (l53, 1), (4, 4): (l44, 1), (5, 4): (l54, 1), (5, 5): (l55, 1),
    }
    outs = coarse_ref.shape[1]
    kind = lax.broadcasted_iota(jnp.int32, (1, outs), 1)
    chosen, sign = jnp.full((1, outs), -1, jnp.int32), jnp.zeros((1, outs), F32)
    for (n, m), (q, way) in entries.items():
        chosen = jnp.where(kind == 6 * m + n, q, chosen)
        sign = jnp.where(kind == 6 * m + n, float(way), sign)
    entry = lax.broadcasted_iota(jnp.int32, (width, outs), 0) % 8
    coarse = jnp.zeros(coarse_ref.shape, F32)
    for base, lines in ((0, low), (8, high)):
        pick = jnp.where(entry + base == chosen, sign, 0.0)
        coarse = coarse + jnp.dot(lines, pick, precision=lax.Precision.HIGHEST, preferred_element_type=F32)
    coarse_ref[...] = coarse

    wait_halo(
        send_sem, side_rows + edge_rows[0], end_rows + start_rows + band_rows + edge_rows[1], corner_rows + edge_rows[2],
        3 * (count - 1),
    )

    some = allsum.at[pl.ds(0, count - 1)]
    pltpu.make_async_copy(some, some, recv_sem.at[TOTALS]).wait()
    if count <= 64:
        lines = [allsum[d] for d in range(count)]
        while len(lines) > 1:
            lines = [a + b for a, b in zip(lines[::2], lines[1::2])] + ([lines[-1]] if len(lines) % 2 else [])
        total = lines[0]
    else:
        total = lax.fori_loop(0, count, lambda d, t: t + allsum[d], jnp.zeros((1, width), F32))
    values = [jnp.broadcast_to(total[:, i : i + 1], shape) for i in range(2 * ITERS)]
    ratios = [values[i + ITERS] / values[i] for i in range(ITERS)]
    growth = ratios[0]
    for i in range(1, ITERS):
        growth = growth * ratios[i]
    scale_ref[0] = ratios[ITERS - 1] * (4.0 / 3.0)
    scale_ref[1] = growth


def finish(raw, fields, iterate, scale, coarse, out_h, probe_h, coarse_h, out, probe, sem):
    weight = scale[0]
    base = {(0, 0): 0, (1, 1): 0, (2, 2): 0, (3, 0): 1, (3, 1): 2}
    for r in range(3):
        base[(4, r)] = 3 + r
        base[(5, r)] = 6 + r
    blocks, modes = raw.shape[:2]
    small = [pltpu.make_async_copy(coarse, coarse_h, sem.at[1]), pltpu.make_async_copy(probe, probe_h, sem.at[2])]
    small[0].start()
    for k in range(blocks):
        for m in range(modes):
            for r in range(3):
                value = raw[k, m, r] * weight
                out[k, m, r] = value + fields[base[(m, r)]] if k == 0 and (m, r) in base else value
        pltpu.make_async_copy(out.at[k], out_h.at[k], sem.at[0]).start()
    for r in range(3):
        probe[r] = iterate[r] * scale[1]
    small[1].start()
    for copy in small + [pltpu.make_async_copy(out, out_h, sem.at[0])]:
        copy.wait()


def local(wide, narrow, coords, member, start_vector, self_block, neighbour_block, neighbours, coarse_map):
    height, width = member.shape
    edge_count = neighbours.shape[0]
    count = wide * narrow
    share = coarse_map.shape[0] // count
    tile = (height, width)
    double = (2 * height, 2 * width)
    planes = 12 + 10 * edge_count
    tiles = edge_slots(planes, width)[1] + 1
    vmem = pltpu.VMEM
    dma = pltpu.SemaphoreType.DMA
    results = (
        jax.ShapeDtypeStruct((edge_count + 1, 6, 3) + tile, F32),
        jax.ShapeDtypeStruct((3,) + tile, F32),
        jax.ShapeDtypeStruct((share, 36), F32),
    )
    staged = pl.pallas_call(
        functools.partial(kernel, wide, narrow, share),
        out_shape=(
            results[0],
            jax.ShapeDtypeStruct((FIELDS,) + tile, F32),
            results[1],
            jax.ShapeDtypeStruct((2,) + tile, F32),
            results[2],
        ),
        in_specs=[pl.BlockSpec(memory_space=pl.ANY)] * 7,
        out_specs=(pl.BlockSpec(memory_space=pltpu.VMEM),) * 5,
        scratch_shapes=[
            vmem((3,) + tile, F32),
            vmem(tile, jnp.int32),
            vmem((edge_count,) + tile, jnp.int32),
            pltpu.SMEM(coarse_map.shape, jnp.int32),
            vmem((planes,) + double, F32),
            vmem((2, tiles) + tile, F32),
            vmem((8, 9) + double, F32),
            vmem((2,) + tile, F32),
            vmem((2, FIELDS, 1, width), F32),
            vmem((FIELDS, 8) + tile, F32),
            vmem((2, width), F32),
            vmem((count, 2, width), F32),
            vmem((1, width), F32),
            vmem((count, 1, width), F32),
            vmem((8, width), F32),
            vmem((4, tiles) + tile, F32),
            vmem((2,) + tile, F32),
            vmem((2, FIELDS, 1, width), F32),
            vmem((4, 1, width), F32),
            vmem((3,) + tile, F32),
            vmem((3,) + tile, F32),
            vmem((max(planes * height, 1024 + 3 * count), 1, width), F32),
            dma((3,)),
            dma(()),
            dma((7,)),
            pltpu.SemaphoreType.REGULAR((len(rounds_of(plane_width(wide), narrow)),)),
        ],
        compiler_params=pltpu.CompilerParams(collective_id=0, has_side_effects=True, vmem_limit_bytes=VMEM_LIMIT),
    )(*(
        pltpu.with_memory_space_constraint(value, pltpu.HBM)
        for value in (
            coords, member, start_vector, self_block.reshape((9,) + tile), neighbour_block.reshape((-1,) + tile),
            neighbours, coarse_map,
        )
    ))
    smoothed, probe, coarse = pl.pallas_call(
        finish,
        out_shape=results,
        in_specs=[pl.BlockSpec(memory_space=pltpu.VMEM)] * 5,
        out_specs=(pl.BlockSpec(memory_space=pl.ANY),) * 3,
        scratch_shapes=[
            vmem(results[0].shape, F32),
            vmem(results[1].shape, F32),
            dma((3,)),
        ],
        compiler_params=pltpu.CompilerParams(vmem_limit_bytes=VMEM_LIMIT),
    )(*staged)
    return smoothed, probe, coarse.T


def solution(mesh):
    return jax.shard_map(
        functools.partial(local, mesh.shape["wide"], mesh.shape["narrow"]),
        mesh=mesh,
        in_specs=(
            P(None, "narrow", "wide"),
            P("narrow", "wide"),
            P(None, "narrow", "wide"),
            P(None, None, "narrow", "wide"),
            P(None, None, None, "narrow", "wide"),
            P(None, "narrow", "wide"),
            P(),
        ),
        out_specs=(
            P(None, None, None, "narrow", "wide"),
            P(None, "narrow", "wide"),
            P(None, ("wide", "narrow")),
        ),
        check_vma=False,
    )
```

```python
import functools

import jax
import jax.numpy as jnp
from jax import lax
from jax.experimental import pallas as pl
from jax.experimental.pallas import tpu as pltpu
from jax.sharding import PartitionSpec as P

TILE = 8
ITERS = 4
MESH = pl.DeviceIdType.MESH
F32 = jnp.float32
SUMS = 10
FIELDS = 9
START, SELF, NB = 0, 3, 12
STENCIL = 81
STEPS = [(-1, -1), (-1, 0), (-1, 1), (0, -1), (0, 1), (1, -1), (1, 0), (1, 1)]
VMEM_LIMIT = 16 * 1024 * 1024


def roll(x, shift, axis):
    size = x.shape[axis]
    shift = shift % size
    return x if shift == 0 else pltpu.roll(x, shift, axis)


def plane_width(wide):
    best = max(size for size in range(1, wide + 1) if wide % size == 0 and size * size <= wide)
    return wide if best == 1 else best


def edge_slots(planes, columns, width):
    per = width // (2 * columns)
    return [(p // per, p % per * 2 * columns) for p in range(planes)], pl.cdiv(planes, per)


def rounds_of(across_plane, narrow):
    def doubled(size):
        steps = [1]
        while 2 * steps[-1] < size:
            steps.append(2 * steps[-1])
        return steps

    return [(0, 1)] + [(step, 0) for step in doubled(across_plane)] + [(0, step) for step in doubled(narrow)[1:]]


IN_NODES, IN_MAP = range(2)
SIDES, CORNERS, BANDS, EDGES, GATHER, TOTALS = range(6)


def kernel(
    wide, narrow, share,
    coords_h, member_h, start_h, self_h, nb_h, nbr_h, cmap_h,
    out_ref, fields, iter_ref, scale_ref, coarse_ref,
    coords, member, nbr, cmap,
    ext, wpack, stencil, pack, tedges, disp, mine, gath, sumrow, allsum, partial,
    cpack, wrecv, erecv, crecv, srecv, htrecv, vtrecv, ctrecv, firsts_own, firsts,
    tally, in_sem, send_sem, recv_sem, round_sem,
):
    count = wide * narrow
    me_w, me_n = lax.axis_index("wide"), lax.axis_index("narrow")
    me = me_w * narrow + me_n
    barrier = pltpu.get_barrier_semaphore()
    across_plane = plane_width(wide)
    plane_count = wide // across_plane
    me_p, me_q = me_w // across_plane, lax.rem(me_w, across_plane)

    height, width = shape = member.shape
    edge_count = nbr.shape[0]
    codes_at = NB + 9 * edge_count
    planes = codes_at + edge_count
    deep = ITERS - 1
    start_slots, _ = edge_slots(SELF, ITERS, width)
    slots, tiles = edge_slots(planes - SELF, deep, width)
    stencil_slots, stencil_tiles = edge_slots(STENCIL, deep, width)
    rounds = rounds_of(across_plane, narrow)
    right, left = 0, 1

    def exists(code):
        dy, dx = STEPS[code]
        ok = None
        for step, at, size in ((dy, me_n, narrow), (dx, me_w, wide)):
            term = at > 0 if step < 0 else (at < size - 1 if step > 0 else None)
            if term is not None:
                ok = term if ok is None else jnp.logical_and(ok, term)
        return ok

    present_at = [exists(code) for code in range(8)]

    def target(code):
        dy, dx = STEPS[code]
        return (me_w + dx, me_n + dy)

    def greet(cond, device):
        @pl.when(cond)
        def _():
            pl.semaphore_signal(barrier, inc=1, device_id=device, device_id_type=MESH)
        return cond.astype(jnp.int32)

    expected = 0
    for code in (1, 6):
        expected = expected + greet(present_at[code], target(code))

    def own(first, size):
        return ext.at[first : first + size, 0:height, 0:width]

    loads = [
        pltpu.make_async_copy(src, dst, in_sem.at[i])
        for src, dst, i in (
            (nb_h, own(NB, nb_h.shape[0]), IN_NODES), (self_h, own(SELF, 9), IN_NODES), (start_h, own(START, 3), IN_NODES),
            (nbr_h, nbr, IN_NODES), (coords_h, coords, IN_NODES), (member_h, member, IN_NODES), (cmap_h, cmap, IN_MAP),
        )
    ]
    for load in loads:
        load.start()

    def wait_rows(sem, rows):
        some = tally.at[0:rows]
        pltpu.make_async_copy(some, some, sem).wait()

    sides_here = (me_w > 0).astype(jnp.int32) + (me_w < wide - 1).astype(jnp.int32)
    ends_here = (me_n > 0).astype(jnp.int32) + (me_n < narrow - 1).astype(jnp.int32)

    def wait_halo(sem, side, end, corner, more=0):
        for a in range(min(wide - 1, 1), min(wide - 1, 2) + 1):
            for b in range(min(narrow - 1, 1), min(narrow - 1, 2) + 1):
                rows = a * side + b * end + a * b * corner + more
                if rows:
                    pl.when(jnp.logical_and(sides_here == a, ends_here == b))(functools.partial(wait_rows, sem, rows))

    for code in (3, 4):
        expected = expected + greet(present_at[code], target(code))

    for p in range(plane_count):
        w = p * across_plane + me_q
        expected = expected + greet(jnp.abs(w - me_w) > 1, (w, me_n))

    def partners(number):
        for way in (-1, 1):
            dq, dn = (way * step for step in rounds[number])
            q, n = me_q + dq, me_n + dn
            yield jnp.logical_and(jnp.logical_and(q >= 0, q < across_plane), jnp.logical_and(n >= 0, n < narrow)), (me_w + dq, n)

    def tell(number):
        for cond, device in partners(number):
            @pl.when(cond)
            def _(device=device):
                pl.semaphore_signal(round_sem.at[number], inc=1, device_id=device, device_id_type=MESH)

    def hear(number):
        pl.semaphore_wait(round_sem.at[number], sum(cond.astype(jnp.int32) for cond, _ in partners(number)))

    def corner_refs(operator, start, low):
        at = 0 if low else height - deep
        start_at = 0 if low else height - ITERS
        return [operator.at[:, at : at + deep, :], start.at[start_at : start_at + ITERS, :]]

    for code in range(8):
        dy, dx = STEPS[code]
        @pl.when(jnp.logical_not(present_at[code]))
        def _(code=code, dy=dy, dx=dx):
            side = right if dx > 0 else left
            if dx == 0:
                at = height if dy > 0 else height + ITERS
                ext[:, at : at + ITERS, 0:width] = jnp.zeros((planes, ITERS, width), F32)
                vtrecv[0 if dy < 0 else 1] = jnp.zeros(vtrecv.shape[1:], F32)
                at = deep - 1 if dy > 0 else height - deep
                firsts[:, at : at + 1, :] = jnp.zeros((3, 1, width), F32)
                erecv[:, at : at + 1, :] = jnp.zeros((tiles, 1, width), F32)
            elif dy == 0:
                wrecv[side] = jnp.zeros(wrecv.shape[1:], F32)
                htrecv[side] = jnp.zeros(htrecv.shape[1:], F32)
            else:
                for ref in corner_refs(crecv.at[side], srecv.at[side], dy > 0):
                    ref[...] = jnp.zeros(ref.shape, F32)
                ctrecv[2 * side + (0 if dy < 0 else 1)] = jnp.zeros(ctrecv.shape[1:], F32)

    lane = lax.broadcasted_iota(jnp.int32, shape, 1)
    row = lax.broadcasted_iota(jnp.int32, shape, 0)
    first, last = lane == 0, lane == width - 1

    pl.semaphore_wait(barrier, expected)
    tell(0)
    wait_rows(in_sem.at[IN_NODES], (planes + 4) * height)
    for k in range(edge_count):
        ext[codes_at + k, 0:height, 0:width] = nbr[k].astype(F32)

    def send(code, pairs, group):
        made = [
            pltpu.make_async_remote_copy(
                src_ref=src, dst_ref=dst, send_sem=send_sem, recv_sem=recv_sem.at[group],
                device_id=target(code), device_id_type=MESH,
            )
            for src, dst in pairs
        ]

        @pl.when(present_at[code])
        def _():
            for copy in made:
                copy.start()

    half = 9 * (edge_count // 2)
    bands = (
        (START, 3, ITERS), (SELF, 9, deep - 1), (NB, half, deep - 1), (NB + half, planes - NB - half, deep - 1),
    )

    def band_pairs(code, band):
        base, size, rows = band
        here, there = (0, height) if STEPS[code][0] < 0 else (height - rows, height + 2 * ITERS - rows)
        return [(
            ext.at[base : base + size, here : here + rows, 0:width],
            ext.at[base : base + size, there : there + rows, 0:width],
        )]

    def end_pairs(code):
        here = deep - 1 if STEPS[code][0] < 0 else height - deep
        return [(wpack.at[0:tiles, here : here + 1, :], erecv.at[:, here : here + 1, :])]

    def first_pairs(code):
        here = deep - 1 if STEPS[code][0] < 0 else height - deep
        return [(firsts_own.at[:, here : here + 1, :], firsts.at[:, here : here + 1, :])]

    for code in (1, 6):
        send(code, band_pairs(code, bands[0]), SIDES)
        send(code, band_pairs(code, bands[1]), BANDS)
    def packed(sources, slots, columns):
        result = []
        for source, (t, at) in zip(sources, slots):
            moved = roll(source(), at + columns, 1)
            if at == 0:
                result.append(moved)
            else:
                result[t] = jnp.where(lane >= at, moved, result[t])
        return result

    def main(p):
        return lambda: ext[p, 0:height, 0:width]

    raw = packed([main(SELF + p) for p in range(planes - SELF)], slots, deep)
    starts = packed([main(START + r) for r in range(SELF)], start_slots, ITERS)
    for t, value in enumerate(raw + starts):
        wpack[t] = value

    for code in (1, 6):
        send(code, end_pairs(code), SIDES)
        send(code, band_pairs(code, bands[2]) + band_pairs(code, bands[3]), BANDS)
    for code in (3, 4):
        send(code, [(wpack, wrecv.at[left if code == 4 else right])], SIDES)

    def by_displacement(r0, c0):
        def at(p):
            return ext[p, r0 : r0 + height, c0 : c0 + width]

        for group in range(0, 8, 2):
            masks = {(code, k): at(codes_at + k) == code for code in (group, group + 1) for k in range(edge_count)}
            for q in range(9):
                blocks = [at(NB + 9 * k + q) for k in range(edge_count)]
                for code in (group, group + 1):
                    value = jnp.zeros(shape, F32)
                    for k in range(edge_count):
                        value = jnp.where(masks[code, k], blocks[k], value)
                    stencil[code, q, r0 : r0 + height, c0 : c0 + width] = value

    def apply(iterate, rs, cs):
        applied = [sum(ext[SELF + 3 * r + s, rs, cs] * iterate[s][rs, cs] for s in range(3)) for r in range(3)]
        for s in range(3):
            for dx in (0, -1, 1):
                shifted = roll(iterate[s], -dx, 1)
                for dy in (-1, 0, 1):
                    if (dy, dx) == (0, 0):
                        continue
                    code = STEPS.index((dy, dx))
                    moved = roll(shifted, -dy, 0)[rs, cs]
                    for r in range(3):
                        applied[r] = applied[r] + stencil[code, 3 * r + s, rs, cs] * moved
        return applied

    by_displacement(0, 0)
    shifted_main = [main(SELF + q) for q in range(9)] + [
        lambda code=code, q=q: stencil[code, q, 0:height, 0:width] for code in range(8) for q in range(9)
    ]
    for t, value in enumerate(packed(shifted_main, stencil_slots, deep)):
        cpack[t] = value
    inside_rows, inside_cols = slice(0, height), slice(0, width)
    applied = apply([ext[START + r, 0:height, 0:width] for r in range(3)], inside_rows, inside_cols)
    for r in range(3):
        firsts_own[r] = applied[r] * (1.0 / ext[SELF + 4 * r, 0:height, 0:width])
    hear(0)
    tell(1)
    for code in (0, 2, 5, 7):
        dy, dx = STEPS[code]
        side = right if dx < 0 else left
        send(code, list(zip(
            corner_refs(cpack, wpack.at[tiles], dy < 0), corner_refs(crecv.at[side], srecv.at[side], dy < 0),
        )), CORNERS)
    for code in (1, 6):
        send(code, first_pairs(code), BANDS)

    present = member[...].astype(F32)
    x, y, z = (coords[r] * present for r in range(3))
    products = [present * present, x * present, y * present, z * present, x * x, y * y, z * z, x * y, x * z, y * z]
    sum_tiles = []
    for base in (0, 8):
        tile = jnp.zeros(shape, F32)
        for q, product in enumerate(products[base : base + 8]):
            tile = jnp.where(row == q, jnp.sum(product, axis=0, keepdims=True), tile)
        for s in (1, 2, 4):
            tile = tile + jnp.where((lane & s) != 0, roll(tile, s, 1), roll(tile, -s, 1))
        sum_tiles.append(tile)
    sums = [sum_tiles[q // 8][q % 8 : q % 8 + 1, :] for q in range(SUMS)]

    def factor(sums):
        n, sx, sy, sz, xx, yy, zz, xy, xz, yz = sums
        l00 = jnp.sqrt(n)
        mx, my, mz = sx / l00, sy / l00, sz / l00
        l33 = jnp.sqrt(xx + yy - mx * mx - my * my)
        l43 = (mx * mz - xz) / l33
        l53 = (my * mz - yz) / l33
        l44 = jnp.sqrt(yy + zz - my * my - mz * mz - l43 * l43)
        l54 = (mx * my - xy - l53 * l43) / l44
        l55 = jnp.sqrt(xx + zz - mx * mx - mz * mz - l53 * l53 - l54 * l54)
        return l00, mx, my, mz, l33, l43, l53, l44, l54, l55

    parts = factor(sums)
    l00, mx, my, mz, l33, l43, l53, l44, l54, l55 = parts
    unit = present / l00
    cx, cy, cz = x - mx * unit, y - my * unit, z - mz * unit
    a0, a1 = -cy / l33, cx / l33
    b0, b1, b2 = -l43 * a0 / l44, (-cz - l43 * a1) / l44, cy / l44
    g0 = (cz - l53 * a0 - l54 * b0) / l55
    g1 = (-l53 * a1 - l54 * b1) / l55
    g2 = (-cx - l54 * b2) / l55
    tent = [unit, a0, a1, b0, b1, b2, g0, g1, g2]
    packl, packr = jnp.zeros(shape, F32), jnp.zeros(shape, F32)
    for j, field in enumerate(tent):
        fields[j] = field
        packl = jnp.where(lane == j, roll(field, j, 1), packl)
        packr = jnp.where(lane == j, roll(field, j + 1, 1), packr)
        tedges[0, j] = field[:1]
        tedges[1, j] = field[height - 1 :]
    pack[left] = packl
    pack[right] = packr
    lane_row = lax.broadcasted_iota(jnp.int32, (1, width), 1) % 8
    rows_out = []
    for base in (0, 8):
        line = jnp.zeros((1, width), F32)
        for q, part in enumerate(parts[base : base + 8]):
            line = jnp.where(lane_row == q, part, line)
        rows_out.append(line)
    mine[0:1] = rows_out[0]
    mine[1:2] = rows_out[1]
    gath[me] = jnp.concatenate(rows_out, axis=0)

    for code in range(8):
        dy, dx = STEPS[code]
        mine_side, their_side = (left, right) if dx < 0 else (right, left)
        if dx == 0:
            src, dst = tedges.at[0 if dy < 0 else 1], vtrecv.at[1 if dy < 0 else 0]
        elif dy == 0:
            src, dst = pack.at[mine_side], htrecv.at[their_side]
        else:
            edge = 0 if dy < 0 else height - 1
            src = pack.at[mine_side, edge : edge + 1, :]
            dst = ctrecv.at[2 * their_side + (1 if dy < 0 else 0)]
        send(code, [(src, dst)], EDGES)

    for number in range(1, len(rounds) - 1):
        hear(number)
        tell(number + 1)
    def joined(from_left, from_right, columns):
        takes_left = lax.rem(lane, 2 * columns) < columns
        return [jnp.where(takes_left, a[...], b[...]) for a, b in zip(from_left, from_right)]

    def tiles_of(ref, count_of):
        return [ref.at[t] for t in range(count_of)]

    def unpack_starts(r0, from_left, from_right):
        both, = joined([from_left], [from_right], ITERS)
        for r, (_, at) in enumerate(start_slots):
            ext[START + r, r0 : r0 + height, width:] = roll(both, -at - ITERS, 1)

    side_rows, start_rows = (tiles + 1) * height, SELF * ITERS
    corner_rows, end_rows = stencil_tiles * deep + ITERS, tiles
    band_rows = (planes - SELF) * (deep - 1) + 3
    edge_rows = (height, FIELDS, 1)
    wait_halo(recv_sem.at[SIDES], side_rows, end_rows + start_rows, 0)
    unpack_starts(0, wrecv.at[left, tiles], wrecv.at[right, tiles])
    both = joined(tiles_of(wrecv.at[left], tiles), tiles_of(wrecv.at[right], tiles), deep)
    for p, (t, at) in enumerate(slots):
        ext[SELF + p, 0:height, width:] = roll(both[t], -at - deep, 1)
        ends = roll(erecv[t], -at - deep, 1)
        ext[SELF + p, height + deep - 1 : height + deep, 0:width] = ends[deep - 1 : deep]
        ext[SELF + p, 2 * height - deep : 2 * height - deep + 1, 0:width] = ends[height - deep : height - deep + 1]
    by_displacement(0, width)

    if len(rounds) > 1:
        hear(len(rounds) - 1)

    def to_all(src, dst, group):
        def one(i):
            k = i // narrow
            w = jnp.where(2 * me_w < wide, wide - 1 - k, k)
            n = lax.rem(me_n + 1 + i, narrow)

            @pl.when(jnp.logical_or(w != me_w, n != me_n))
            def _():
                pltpu.make_async_remote_copy(
                    src_ref=src, dst_ref=dst, send_sem=send_sem, recv_sem=recv_sem.at[group],
                    device_id=(w, n), device_id_type=MESH,
                ).start()

        if count <= 64:
            for i in range(count):
                one(i)
        else:
            pl.loop(0, count)(one)

    to_all(mine, gath.at[me], GATHER)

    wait_halo(recv_sem.at[CORNERS], 0, 0, corner_rows)
    unpack_starts(height, srecv.at[left], srecv.at[right])
    both = joined(tiles_of(crecv.at[left], stencil_tiles), tiles_of(crecv.at[right], stencil_tiles), deep)
    for p, (t, at) in enumerate(stencil_slots):
        value = roll(both[t], -at - deep, 1)
        if p < 9:
            ext[SELF + p, height:, width:] = value
        else:
            stencil[(p - 9) // 9, (p - 9) % 9, height:, width:] = value
    whole_cols, beyond = slice(None), slice(width, None)
    begin = [ext[START + r] for r in range(3)]
    begin_top = apply(begin, inside_rows, whole_cols)
    begin_corner = apply(begin, slice(height, None), beyond)
    wait_halo(recv_sem.at[BANDS], 0, band_rows, 0)
    by_displacement(height, 0)

    def full(p):
        return ext[p]

    selfb = {(r, s): (lambda r=r, s=s: ext[SELF + 3 * r + s, 0:height, 0:width]) for r in range(3) for s in range(3)}
    nb = {
        (k, r, s): (lambda k=k, r=r, s=s: ext[NB + 9 * k + 3 * r + s, 0:height, 0:width])
        for k in range(edge_count) for r in range(3) for s in range(3)
    }
    elane = lax.broadcasted_iota(jnp.int32, (2 * height, 2 * width), 1)
    erow = lax.broadcasted_iota(jnp.int32, (2 * height, 2 * width), 0)

    last_row = jnp.where(me_n < narrow - 1, height + ITERS, height)
    back_row = jnp.where(me_n > 0, height + ITERS, 2 * height)
    last_lane = jnp.where(me_w < wide - 1, width + ITERS, width)
    back_lane = jnp.where(me_w > 0, 2 * width - ITERS, 2 * width)
    inside = jnp.logical_and(
        jnp.logical_or(erow < last_row, erow >= back_row), jnp.logical_or(elane < last_lane, elane >= back_lane)
    )
    inverse = [jnp.where(inside, 1.0 / full(SELF + 4 * r), 0.0) for r in range(3)]
    diag = [selfb[r, r]() for r in range(3)]
    inv = [inverse[r][:height, :width] for r in range(3)]

    sent = jnp.logical_and(
        jnp.logical_or(erow == height + deep - 1, erow == 2 * height - deep),
        jnp.logical_and(elane > 0, elane < width - 1),
    )
    spread = [
        jnp.concatenate([jnp.concatenate([firsts[r], firsts[r]], axis=0)] * 2, axis=1) for r in range(3)
    ]
    iterate = begin
    for number in range(ITERS):
        final = number == ITERS - 1
        rs, cs = (slice(0, height), slice(0, width)) if final else (slice(None), slice(None))
        if number == 0:
            outer = apply(begin, slice(height, None), inside_cols)
            applied = [
                jnp.concatenate([begin_top[r], jnp.concatenate([outer[r], begin_corner[r]], axis=1)], axis=0) for r in range(3)
            ]
        else:
            applied = apply(iterate, rs, cs)
        mine_it = [v[:height, :width] for v in iterate]
        mine_ap = [v[:height, :width] for v in applied]
        curvature = sum(mine_it[r] * mine_ap[r] for r in range(3))
        energy = sum(mine_it[r] * diag[r] * mine_it[r] for r in range(3))
        partial[number : number + 1] = jnp.sum(curvature, axis=0, keepdims=True)
        partial[number + 4 : number + 5] = jnp.sum(energy, axis=0, keepdims=True)
        iterate = [applied[r] * (inv[r] if final else inverse[r]) for r in range(3)]
        if number == 0:
            iterate = [jnp.where(sent, spread[r], iterate[r]) for r in range(3)]

    totals = jnp.sum(partial[...], axis=1, keepdims=True)
    line = jnp.sum(jnp.where(lane == row, totals, 0.0), axis=0, keepdims=True)
    sumrow[...] = line
    allsum[me] = line
    to_all(sumrow, allsum.at[me], TOTALS)

    for r in range(3):
        iter_ref[r] = iterate[r]

    wait_halo(recv_sem.at[EDGES], *edge_rows)

    top, bottom = row == 0, row == height - 1
    lcol, rcol = htrecv[left], htrecv[right]
    corner_l = jnp.where(bottom, ctrecv[2 * left], ctrecv[2 * left + 1])
    corner_r = jnp.where(bottom, ctrecv[2 * right], ctrecv[2 * right + 1])
    for j in range(FIELDS):
        v = tent[j]
        w = jnp.where(bottom, vtrecv[0, j], vtrecv[1, j])
        vl = jnp.where(first, roll(lcol, -j, 1), roll(v, 1, 1))
        vr = jnp.where(last, roll(rcol, width - 1 - j, 1), roll(v, -1, 1))
        wl = jnp.where(first, roll(corner_l, -j, 1), roll(w, 1, 1))
        wr = jnp.where(last, roll(corner_r, width - 1 - j, 1), roll(w, -1, 1))
        pairs = ((vl, wl), (v, w), (vr, wr))
        up = [roll(jnp.where(bottom, b, a), 1, 0) for a, b in pairs]
        down = [roll(jnp.where(top, b, a), -1, 0) for a, b in pairs]
        for code, moved in enumerate(up + [vl, vr] + down):
            disp[j, code] = moved

    def piece(block, picked, index):
        unit, a0, a1, b0, b1, b2, g0, g1, g2 = picked
        for r in range(3):
            c0, c1, c2 = (block(r, s) * -inv[r] for s in range(3))
            out_ref[index, 0, r] = c0 * unit
            out_ref[index, 1, r] = c1 * unit
            out_ref[index, 2, r] = c2 * unit
            out_ref[index, 3, r] = c0 * a0 + c1 * a1
            out_ref[index, 4, r] = c0 * b0 + c1 * b1 + c2 * b2
            out_ref[index, 5, r] = c0 * g0 + c1 * g1 + c2 * g2

    piece(lambda r, s: selfb[r, s](), [fields[j] for j in range(FIELDS)], 0)
    for k in range(edge_count):
        masks = [nbr[k] == code for code in range(1, 8)]
        picked = []
        for j in range(FIELDS):
            value = disp[j, 0]
            for code in range(1, 8):
                value = jnp.where(masks[code - 1], disp[j, code], value)
            picked.append(value)
        piece(lambda r, s: nb[k, r, s](), picked, k + 1)

    loads[6].wait()
    some = gath.at[pl.ds(0, count - 1)]
    pltpu.make_async_copy(some, some, recv_sem.at[GATHER]).wait()
    across = width // TILE * wide
    tiles_x, tiles_y = width // TILE, height // TILE
    crow = lax.broadcasted_iota(jnp.int32, (share, width), 0)
    cgroup = lax.broadcasted_iota(jnp.int32, (share, width), 1) // TILE
    low, high = jnp.zeros((share, width), F32), jnp.zeros((share, width), F32)
    for j in range(share):
        wanted = cmap[me * share + j]
        tile_row, tile_col = wanted // across, lax.rem(wanted, across)
        slot = tile_col // tiles_x * narrow + tile_row // tiles_y
        lines = gath[slot]
        take = jnp.logical_and(crow == j, cgroup == lax.rem(tile_col, tiles_x))
        low = jnp.where(take, lines[0:1], low)
        high = jnp.where(take, lines[1:2], high)
    l00, mx, my, mz, l33, l43, l53, l44, l54, l55 = range(SUMS)
    entries = {
        (0, 0): (l00, 1), (1, 1): (l00, 1), (2, 2): (l00, 1),
        (3, 0): (my, -1), (3, 1): (mx, 1), (4, 1): (mz, -1), (4, 2): (my, 1), (5, 0): (mz, 1), (5, 2): (mx, -1),
        (3, 3): (l33, 1), (4, 3): (l43, 1), (5, 3): (l53, 1), (4, 4): (l44, 1), (5, 4): (l54, 1), (5, 5): (l55, 1),
    }
    outs = coarse_ref.shape[1]
    kind = lax.broadcasted_iota(jnp.int32, (1, outs), 1)
    chosen, sign = jnp.full((1, outs), -1, jnp.int32), jnp.zeros((1, outs), F32)
    for (n, m), (q, way) in entries.items():
        chosen = jnp.where(kind == 6 * m + n, q, chosen)
        sign = jnp.where(kind == 6 * m + n, float(way), sign)
    entry = lax.broadcasted_iota(jnp.int32, (width, outs), 0) % 8
    coarse = jnp.zeros(coarse_ref.shape, F32)
    for base, lines in ((0, low), (8, high)):
        pick = jnp.where(entry + base == chosen, sign, 0.0)
        coarse = coarse + jnp.dot(lines, pick, precision=lax.Precision.HIGHEST, preferred_element_type=F32)
    coarse_ref[...] = coarse

    wait_halo(
        send_sem, side_rows + edge_rows[0], end_rows + start_rows + band_rows + edge_rows[1], corner_rows + edge_rows[2],
        3 * (count - 1),
    )

    some = allsum.at[pl.ds(0, count - 1)]
    pltpu.make_async_copy(some, some, recv_sem.at[TOTALS]).wait()
    if count <= 64:
        lines = [allsum[d] for d in range(count)]
        while len(lines) > 1:
            lines = [a + b for a, b in zip(lines[::2], lines[1::2])] + ([lines[-1]] if len(lines) % 2 else [])
        total = lines[0]
    else:
        total = lax.fori_loop(0, count, lambda d, t: t + allsum[d], jnp.zeros((1, width), F32))
    values = [jnp.broadcast_to(total[:, i : i + 1], shape) for i in range(2 * ITERS)]
    ratios = [values[i + ITERS] / values[i] for i in range(ITERS)]
    growth = ratios[0]
    for i in range(1, ITERS):
        growth = growth * ratios[i]
    scale_ref[0] = ratios[ITERS - 1] * (4.0 / 3.0)
    scale_ref[1] = growth


def finish(raw, fields, iterate, scale, coarse, out_h, probe_h, coarse_h, out, probe, sem):
    weight = scale[0]
    base = {(0, 0): 0, (1, 1): 0, (2, 2): 0, (3, 0): 1, (3, 1): 2}
    for r in range(3):
        base[(4, r)] = 3 + r
        base[(5, r)] = 6 + r
    blocks, modes = raw.shape[:2]
    small = [pltpu.make_async_copy(coarse, coarse_h, sem.at[1]), pltpu.make_async_copy(probe, probe_h, sem.at[2])]
    small[0].start()
    for k in range(blocks):
        for m in range(modes):
            for r in range(3):
                value = raw[k, m, r] * weight
                out[k, m, r] = value + fields[base[(m, r)]] if k == 0 and (m, r) in base else value
        pltpu.make_async_copy(out.at[k], out_h.at[k], sem.at[0]).start()
    for r in range(3):
        probe[r] = iterate[r] * scale[1]
    small[1].start()
    for copy in small + [pltpu.make_async_copy(out, out_h, sem.at[0])]:
        copy.wait()


def local(wide, narrow, coords, member, start_vector, self_block, neighbour_block, neighbours, coarse_map):
    height, width = member.shape
    edge_count = neighbours.shape[0]
    count = wide * narrow
    share = coarse_map.shape[0] // count
    tile = (height, width)
    double = (2 * height, 2 * width)
    planes = 12 + 10 * edge_count
    tiles = edge_slots(planes - SELF, ITERS - 1, width)[1]
    stencil_tiles = edge_slots(STENCIL, ITERS - 1, width)[1]
    vmem = pltpu.VMEM
    dma = pltpu.SemaphoreType.DMA
    results = (
        jax.ShapeDtypeStruct((edge_count + 1, 6, 3) + tile, F32),
        jax.ShapeDtypeStruct((3,) + tile, F32),
        jax.ShapeDtypeStruct((share, 36), F32),
    )
    staged = pl.pallas_call(
        functools.partial(kernel, wide, narrow, share),
        out_shape=(
            results[0],
            jax.ShapeDtypeStruct((FIELDS,) + tile, F32),
            results[1],
            jax.ShapeDtypeStruct((2,) + tile, F32),
            results[2],
        ),
        in_specs=[pl.BlockSpec(memory_space=pl.ANY)] * 7,
        out_specs=(pl.BlockSpec(memory_space=pltpu.VMEM),) * 5,
        scratch_shapes=[
            vmem((3,) + tile, F32),
            vmem(tile, jnp.int32),
            vmem((edge_count,) + tile, jnp.int32),
            pltpu.SMEM(coarse_map.shape, jnp.int32),
            vmem((planes,) + double, F32),
            vmem((tiles + 1,) + tile, F32),
            vmem((8, 9) + double, F32),
            vmem((2,) + tile, F32),
            vmem((2, FIELDS, 1, width), F32),
            vmem((FIELDS, 8) + tile, F32),
            vmem((2, width), F32),
            vmem((count, 2, width), F32),
            vmem((1, width), F32),
            vmem((count, 1, width), F32),
            vmem((8, width), F32),
            vmem((stencil_tiles,) + tile, F32),
            vmem((2, tiles + 1) + tile, F32),
            vmem((tiles,) + tile, F32),
            vmem((2, stencil_tiles) + tile, F32),
            vmem((2,) + tile, F32),
            vmem((2,) + tile, F32),
            vmem((2, FIELDS, 1, width), F32),
            vmem((4, 1, width), F32),
            vmem((3,) + tile, F32),
            vmem((3,) + tile, F32),
            vmem((max((planes + 4) * height, 1024 + 3 * count), 1, width), F32),
            dma((2,)),
            dma(()),
            dma((6,)),
            pltpu.SemaphoreType.REGULAR((len(rounds_of(plane_width(wide), narrow)),)),
        ],
        compiler_params=pltpu.CompilerParams(collective_id=0, has_side_effects=True, vmem_limit_bytes=VMEM_LIMIT),
    )(*(
        pltpu.with_memory_space_constraint(value, pltpu.HBM)
        for value in (
            coords, member, start_vector, self_block.reshape((9,) + tile), neighbour_block.reshape((-1,) + tile),
            neighbours, coarse_map,
        )
    ))
    smoothed, probe, coarse = pl.pallas_call(
        finish,
        out_shape=results,
        in_specs=[pl.BlockSpec(memory_space=pltpu.VMEM)] * 5,
        out_specs=(pl.BlockSpec(memory_space=pl.ANY),) * 3,
        scratch_shapes=[
            vmem(results[0].shape, F32),
            vmem(results[1].shape, F32),
            dma((3,)),
        ],
        compiler_params=pltpu.CompilerParams(vmem_limit_bytes=VMEM_LIMIT),
    )(*staged)
    return smoothed, probe, coarse.T


def solution(mesh):
    return jax.shard_map(
        functools.partial(local, mesh.shape["wide"], mesh.shape["narrow"]),
        mesh=mesh,
        in_specs=(
            P(None, "narrow", "wide"),
            P("narrow", "wide"),
            P(None, "narrow", "wide"),
            P(None, None, "narrow", "wide"),
            P(None, None, None, "narrow", "wide"),
            P(None, "narrow", "wide"),
            P(),
        ),
        out_specs=(
            P(None, None, None, "narrow", "wide"),
            P(None, "narrow", "wide"),
            P(None, ("wide", "narrow")),
        ),
        check_vma=False,
    )
```

```python
import functools

import jax
import jax.numpy as jnp
from jax import lax
from jax.experimental import pallas as pl
from jax.experimental.pallas import tpu as pltpu
from jax.sharding import PartitionSpec as P

TILE = 8
ITERS = 4
MESH = pl.DeviceIdType.MESH
F32 = jnp.float32
SUMS = 10
FIELDS = 9
START, SELF, NB = 0, 3, 12
STENCIL = 81
STEPS = [(-1, -1), (-1, 0), (-1, 1), (0, -1), (0, 1), (1, -1), (1, 0), (1, 1)]
VMEM_LIMIT = 16 * 1024 * 1024


def roll(x, shift, axis):
    size = x.shape[axis]
    shift = shift % size
    return x if shift == 0 else pltpu.roll(x, shift, axis)


def plane_width(wide):
    best = max(size for size in range(1, wide + 1) if wide % size == 0 and size * size <= wide)
    return wide if best == 1 else best


def edge_slots(planes, columns, width):
    per = width // (2 * columns)
    return [(p // per, p % per * 2 * columns) for p in range(planes)], pl.cdiv(planes, per)


def rounds_of(across_plane, narrow):
    def doubled(size):
        steps = [1]
        while 2 * steps[-1] < size:
            steps.append(2 * steps[-1])
        return steps

    return [(0, 1)] + [(step, 0) for step in doubled(across_plane)] + [(0, step) for step in doubled(narrow)[1:]]


IN_NODES, IN_MAP = range(2)
SIDES, ENDS, CORNERS, BANDS, EDGES, GATHER, TOTALS = range(7)


def kernel(
    wide, narrow, share,
    coords_h, member_h, start_h, self_h, nb_h, nbr_h, cmap_h,
    out_ref, fields, iter_ref, scale_ref, coarse_ref,
    coords, member, nbr, cmap,
    ext, wpack, stencil, pack, tedges, disp, mine, gath, sumrow, allsum, partial,
    cpack, wrecv, erecv, crecv, srecv, near, nrecv, htrecv, vtrecv, ctrecv, firsts_own, firsts,
    tally, in_sem, send_sem, recv_sem, round_sem,
):
    count = wide * narrow
    me_w, me_n = lax.axis_index("wide"), lax.axis_index("narrow")
    me = me_w * narrow + me_n
    barrier = pltpu.get_barrier_semaphore()
    across_plane = plane_width(wide)
    plane_count = wide // across_plane
    me_p, me_q = me_w // across_plane, lax.rem(me_w, across_plane)

    height, width = shape = member.shape
    edge_count = nbr.shape[0]
    codes_at = NB + 9 * edge_count
    planes = codes_at + edge_count
    deep = ITERS - 1
    start_slots, _ = edge_slots(SELF, ITERS, width)
    slots, tiles = edge_slots(planes - SELF, deep, width)
    stencil_slots, stencil_tiles = edge_slots(STENCIL, deep, width)
    rounds = rounds_of(across_plane, narrow)
    right, left = 0, 1

    def exists(code):
        dy, dx = STEPS[code]
        ok = None
        for step, at, size in ((dy, me_n, narrow), (dx, me_w, wide)):
            term = at > 0 if step < 0 else (at < size - 1 if step > 0 else None)
            if term is not None:
                ok = term if ok is None else jnp.logical_and(ok, term)
        return ok

    present_at = [exists(code) for code in range(8)]

    def target(code):
        dy, dx = STEPS[code]
        return (me_w + dx, me_n + dy)

    def greet(cond, device):
        @pl.when(cond)
        def _():
            pl.semaphore_signal(barrier, inc=1, device_id=device, device_id_type=MESH)
        return cond.astype(jnp.int32)

    expected = 0
    for code in (1, 6):
        expected = expected + greet(present_at[code], target(code))

    def own(first, size):
        return ext.at[first : first + size, 0:height, 0:width]

    loads = [
        pltpu.make_async_copy(src, dst, in_sem.at[i])
        for src, dst, i in (
            (nb_h, own(NB, nb_h.shape[0]), IN_NODES), (self_h, own(SELF, 9), IN_NODES), (start_h, own(START, 3), IN_NODES),
            (nbr_h, nbr, IN_NODES), (coords_h, coords, IN_NODES), (member_h, member, IN_NODES), (cmap_h, cmap, IN_MAP),
        )
    ]
    for load in loads:
        load.start()

    def wait_rows(sem, rows):
        some = tally.at[0:rows]
        pltpu.make_async_copy(some, some, sem).wait()

    sides_here = (me_w > 0).astype(jnp.int32) + (me_w < wide - 1).astype(jnp.int32)
    ends_here = (me_n > 0).astype(jnp.int32) + (me_n < narrow - 1).astype(jnp.int32)

    def wait_halo(sem, side, end, corner, more=0):
        for a in range(min(wide - 1, 1), min(wide - 1, 2) + 1):
            for b in range(min(narrow - 1, 1), min(narrow - 1, 2) + 1):
                rows = a * side + b * end + a * b * corner + more
                if rows:
                    pl.when(jnp.logical_and(sides_here == a, ends_here == b))(functools.partial(wait_rows, sem, rows))

    for code in (3, 4):
        expected = expected + greet(present_at[code], target(code))

    for p in range(plane_count):
        w = p * across_plane + me_q
        expected = expected + greet(jnp.abs(w - me_w) > 1, (w, me_n))

    def partners(number):
        for way in (-1, 1):
            dq, dn = (way * step for step in rounds[number])
            q, n = me_q + dq, me_n + dn
            yield jnp.logical_and(jnp.logical_and(q >= 0, q < across_plane), jnp.logical_and(n >= 0, n < narrow)), (me_w + dq, n)

    def tell(number):
        for cond, device in partners(number):
            @pl.when(cond)
            def _(device=device):
                pl.semaphore_signal(round_sem.at[number], inc=1, device_id=device, device_id_type=MESH)

    def hear(number):
        pl.semaphore_wait(round_sem.at[number], sum(cond.astype(jnp.int32) for cond, _ in partners(number)))

    def corner_refs(operator, start, low):
        at = 0 if low else height - deep
        start_at = 0 if low else height - ITERS
        return [operator.at[:, at : at + deep, :], start.at[start_at : start_at + ITERS, :]]

    for side, at in ((0, 1), (1, height - 2)):
        nrecv[side, :, 0:at, :] = jnp.zeros((near.shape[0], at, width), F32)
        nrecv[side, :, at + 1 :, :] = jnp.zeros((near.shape[0], height - at - 1, width), F32)
    for code in range(8):
        dy, dx = STEPS[code]
        @pl.when(jnp.logical_not(present_at[code]))
        def _(code=code, dy=dy, dx=dx):
            side = right if dx > 0 else left
            if dx == 0:
                at = height if dy > 0 else height + ITERS
                ext[:, at : at + ITERS, 0:width] = jnp.zeros((planes, ITERS, width), F32)
                vtrecv[0 if dy < 0 else 1] = jnp.zeros(vtrecv.shape[1:], F32)
                at = 1 if dy > 0 else height - deep
                firsts[:, at : at + deep - 1, :] = jnp.zeros((3, deep - 1, width), F32)
                erecv[:, at : at + deep - 1, :] = jnp.zeros((tiles, deep - 1, width), F32)
                at = 1 if dy > 0 else height - 2
                nrecv[0 if dy > 0 else 1, :, at : at + 1, :] = jnp.zeros((near.shape[0], 1, width), F32)
            elif dy == 0:
                wrecv[side] = jnp.zeros(wrecv.shape[1:], F32)
                htrecv[side] = jnp.zeros(htrecv.shape[1:], F32)
            else:
                for ref in corner_refs(crecv.at[side], srecv.at[side], dy > 0):
                    ref[...] = jnp.zeros(ref.shape, F32)
                ctrecv[2 * side + (0 if dy < 0 else 1)] = jnp.zeros(ctrecv.shape[1:], F32)

    lane = lax.broadcasted_iota(jnp.int32, shape, 1)
    row = lax.broadcasted_iota(jnp.int32, shape, 0)
    first, last = lane == 0, lane == width - 1

    pl.semaphore_wait(barrier, expected)
    tell(0)
    wait_rows(in_sem.at[IN_NODES], (planes + 4) * height)
    for k in range(edge_count):
        ext[codes_at + k, 0:height, 0:width] = nbr[k].astype(F32)

    def send(code, pairs, group):
        made = [
            pltpu.make_async_remote_copy(
                src_ref=src, dst_ref=dst, send_sem=send_sem, recv_sem=recv_sem.at[group],
                device_id=target(code), device_id_type=MESH,
            )
            for src, dst in pairs
        ]

        @pl.when(present_at[code])
        def _():
            for copy in made:
                copy.start()

    bands = ((START, 3, ITERS), (SELF, 9, 1), (NB, planes - NB, 1))

    def band_pairs(code, band):
        base, size, rows = band
        here, there = (0, height) if STEPS[code][0] < 0 else (height - rows, height + 2 * ITERS - rows)
        return [(
            ext.at[base : base + size, here : here + rows, 0:width],
            ext.at[base : base + size, there : there + rows, 0:width],
        )]

    def far_rows(code):
        at = 1 if STEPS[code][0] < 0 else height - deep
        return slice(at, at + deep - 1)

    def end_pairs(code):
        at = far_rows(code)
        return [(wpack.at[0:tiles, at, :], erecv.at[:, at, :])]

    def first_pairs(code):
        at = far_rows(code)
        return [(firsts_own.at[:, at, :], firsts.at[:, at, :])]

    def near_pairs(code):
        at = 1 if STEPS[code][0] < 0 else height - 2
        return [(near.at[:, at : at + 1, :], nrecv.at[0 if code == 1 else 1, :, at : at + 1, :])]

    for code in (1, 6):
        send(code, band_pairs(code, bands[0]), ENDS)
        send(code, band_pairs(code, bands[1]), BANDS)
    def packed(sources, slots, columns):
        result = []
        for source, (t, at) in zip(sources, slots):
            moved = roll(source(), at + columns, 1)
            if at == 0:
                result.append(moved)
            else:
                result[t] = jnp.where(lane >= at, moved, result[t])
        return result

    def main(p):
        return lambda: ext[p, 0:height, 0:width]

    raw = packed([main(SELF + p) for p in range(planes - SELF)], slots, deep)
    starts = packed([main(START + r) for r in range(SELF)], start_slots, ITERS)
    for t, value in enumerate(raw + starts):
        wpack[t] = value

    for code in (1, 6):
        send(code, end_pairs(code), ENDS)
        send(code, band_pairs(code, bands[2]), BANDS)
    for code in (3, 4):
        send(code, [(wpack, wrecv.at[left if code == 4 else right])], SIDES)

    def by_displacement(r0, c0, sent=None):
        def at(p):
            return ext[p, r0 : r0 + height, c0 : c0 + width]

        for group in range(0, 8, 2):
            masks = {(code, k): at(codes_at + k) == code for code in (group, group + 1) for k in range(edge_count)}
            for q in range(9):
                blocks = [at(NB + 9 * k + q) for k in range(edge_count)]
                for code in (group, group + 1):
                    value = jnp.zeros(shape, F32)
                    if sent is not None and code in (0, 1, 2):
                        value = sent[0, 9 * code + q]
                    elif sent is not None and code in (5, 6, 7):
                        value = sent[1, 9 * (code - 5) + q]
                    for k in range(edge_count):
                        value = jnp.where(masks[code, k], blocks[k], value)
                    stencil[code, q, r0 : r0 + height, c0 : c0 + width] = value

    def apply_parts(iterate, rs, cs, split):
        parts = {0: [sum(ext[SELF + 3 * r + s, rs, cs] * iterate[s][rs, cs] for s in range(3)) for r in range(3)]}
        for s in range(3):
            for dx in (0, -1, 1):
                shifted = roll(iterate[s], -dx, 1)
                for dy in (-1, 0, 1):
                    if (dy, dx) == (0, 0):
                        continue
                    code = STEPS.index((dy, dx))
                    moved = roll(shifted, -dy, 0)[rs, cs]
                    part = parts.setdefault(dy if split else 0, [None] * 3)
                    for r in range(3):
                        term = stencil[code, 3 * r + s, rs, cs] * moved
                        part[r] = term if part[r] is None else part[r] + term
        return parts

    def apply(iterate, rs, cs):
        return apply_parts(iterate, rs, cs, False)[0]

    by_displacement(0, 0)
    inside_rows, inside_cols = slice(0, height), slice(0, width)
    own_inverse = [1.0 / ext[SELF + 4 * r, 0:height, 0:width] for r in range(3)]
    applied = apply([ext[START + r, 0:height, 0:width] for r in range(3)], inside_rows, inside_cols)
    first_own = [applied[r] * own_inverse[r] for r in range(3)]
    for r in range(3):
        firsts_own[r] = first_own[r]
    known = jnp.logical_and(lane > 1, lane < width - 2)
    upper = row < height // 2
    scale = [jnp.where(known, own_inverse[r], 0.0) for r in range(3)]
    for c in range(3):
        for q in range(9):
            toward = jnp.where(upper, stencil[c, q, 0:height, 0:width], stencil[c + 5, q, 0:height, 0:width])
            near[9 * c + q] = jnp.where(known, toward * scale[q // 3], 0.0)
    split = apply_parts(first_own, inside_rows, inside_cols, True)
    for r in range(3):
        second = split[0][r] + jnp.where(upper, split[1][r], split[-1][r])
        near[27 + r] = jnp.where(known, second * own_inverse[r], 0.0)
    for code in (1, 6):
        send(code, first_pairs(code) + near_pairs(code), BANDS)

    shifted_main = [main(SELF + q) for q in range(9)] + [
        lambda code=code, q=q: stencil[code, q, 0:height, 0:width] for code in range(8) for q in range(9)
    ]
    for t, value in enumerate(packed(shifted_main, stencil_slots, deep)):
        cpack[t] = value
    hear(0)
    tell(1)
    for code in (0, 2, 5, 7):
        dy, dx = STEPS[code]
        side = right if dx < 0 else left
        send(code, list(zip(
            corner_refs(cpack, wpack.at[tiles], dy < 0), corner_refs(crecv.at[side], srecv.at[side], dy < 0),
        )), CORNERS)

    present = member[...].astype(F32)
    x, y, z = (coords[r] * present for r in range(3))
    products = [present * present, x * present, y * present, z * present, x * x, y * y, z * z, x * y, x * z, y * z]
    sum_tiles = []
    for base in (0, 8):
        tile = jnp.zeros(shape, F32)
        for q, product in enumerate(products[base : base + 8]):
            tile = jnp.where(row == q, jnp.sum(product, axis=0, keepdims=True), tile)
        for s in (1, 2, 4):
            tile = tile + jnp.where((lane & s) != 0, roll(tile, s, 1), roll(tile, -s, 1))
        sum_tiles.append(tile)
    sums = [sum_tiles[q // 8][q % 8 : q % 8 + 1, :] for q in range(SUMS)]

    def factor(sums):
        n, sx, sy, sz, xx, yy, zz, xy, xz, yz = sums
        l00 = jnp.sqrt(n)
        mx, my, mz = sx / l00, sy / l00, sz / l00
        l33 = jnp.sqrt(xx + yy - mx * mx - my * my)
        l43 = (mx * mz - xz) / l33
        l53 = (my * mz - yz) / l33
        l44 = jnp.sqrt(yy + zz - my * my - mz * mz - l43 * l43)
        l54 = (mx * my - xy - l53 * l43) / l44
        l55 = jnp.sqrt(xx + zz - mx * mx - mz * mz - l53 * l53 - l54 * l54)
        return l00, mx, my, mz, l33, l43, l53, l44, l54, l55

    parts = factor(sums)
    l00, mx, my, mz, l33, l43, l53, l44, l54, l55 = parts
    unit = present / l00
    cx, cy, cz = x - mx * unit, y - my * unit, z - mz * unit
    a0, a1 = -cy / l33, cx / l33
    b0, b1, b2 = -l43 * a0 / l44, (-cz - l43 * a1) / l44, cy / l44
    g0 = (cz - l53 * a0 - l54 * b0) / l55
    g1 = (-l53 * a1 - l54 * b1) / l55
    g2 = (-cx - l54 * b2) / l55
    tent = [unit, a0, a1, b0, b1, b2, g0, g1, g2]
    packl, packr = jnp.zeros(shape, F32), jnp.zeros(shape, F32)
    for j, field in enumerate(tent):
        fields[j] = field
        packl = jnp.where(lane == j, roll(field, j, 1), packl)
        packr = jnp.where(lane == j, roll(field, j + 1, 1), packr)
        tedges[0, j] = field[:1]
        tedges[1, j] = field[height - 1 :]
    pack[left] = packl
    pack[right] = packr
    lane_row = lax.broadcasted_iota(jnp.int32, (1, width), 1) % 8
    rows_out = []
    for base in (0, 8):
        line = jnp.zeros((1, width), F32)
        for q, part in enumerate(parts[base : base + 8]):
            line = jnp.where(lane_row == q, part, line)
        rows_out.append(line)
    mine[0:1] = rows_out[0]
    mine[1:2] = rows_out[1]
    gath[me] = jnp.concatenate(rows_out, axis=0)

    for code in range(8):
        dy, dx = STEPS[code]
        mine_side, their_side = (left, right) if dx < 0 else (right, left)
        if dx == 0:
            src, dst = tedges.at[0 if dy < 0 else 1], vtrecv.at[1 if dy < 0 else 0]
        elif dy == 0:
            src, dst = pack.at[mine_side], htrecv.at[their_side]
        else:
            edge = 0 if dy < 0 else height - 1
            src = pack.at[mine_side, edge : edge + 1, :]
            dst = ctrecv.at[2 * their_side + (1 if dy < 0 else 0)]
        send(code, [(src, dst)], EDGES)

    for number in range(1, len(rounds) - 1):
        hear(number)
        tell(number + 1)
    if len(rounds) > 1:
        hear(len(rounds) - 1)

    def to_all(src, dst, group):
        def one(i):
            k = i // narrow
            w = jnp.where(2 * me_w < wide, wide - 1 - k, k)
            n = lax.rem(me_n + 1 + i, narrow)

            @pl.when(jnp.logical_or(w != me_w, n != me_n))
            def _():
                pltpu.make_async_remote_copy(
                    src_ref=src, dst_ref=dst, send_sem=send_sem, recv_sem=recv_sem.at[group],
                    device_id=(w, n), device_id_type=MESH,
                ).start()

        if count <= 64:
            for i in range(count):
                one(i)
        else:
            pl.loop(0, count)(one)

    to_all(mine, gath.at[me], GATHER)

    def joined(from_left, from_right, columns):
        takes_left = lax.rem(lane, 2 * columns) < columns
        return [jnp.where(takes_left, a[...], b[...]) for a, b in zip(from_left, from_right)]

    def tiles_of(ref, count_of):
        return [ref.at[t] for t in range(count_of)]

    def unpack_starts(r0, from_left, from_right):
        both, = joined([from_left], [from_right], ITERS)
        for r, (_, at) in enumerate(start_slots):
            ext[START + r, r0 : r0 + height, width:] = roll(both, -at - ITERS, 1)

    side_rows, start_rows = (tiles + 1) * height, SELF * ITERS
    corner_rows, end_rows = stencil_tiles * deep + ITERS, tiles * (deep - 1)
    band_rows = planes - SELF + 3 * (deep - 1) + near.shape[0]
    edge_rows = (height, FIELDS, 1)
    wait_halo(recv_sem.at[SIDES], side_rows, 0, 0)
    unpack_starts(0, wrecv.at[left, tiles], wrecv.at[right, tiles])
    both = joined(tiles_of(wrecv.at[left], tiles), tiles_of(wrecv.at[right], tiles), deep)
    for p, (t, at) in enumerate(slots):
        ext[SELF + p, 0:height, width:] = roll(both[t], -at - deep, 1)
    by_displacement(0, width)
    wait_halo(recv_sem.at[ENDS], 0, end_rows + start_rows, 0)
    for p, (t, at) in enumerate(slots):
        ends = roll(erecv[t], -at - deep, 1)
        if p < 9 or p >= codes_at - SELF:
            ends = jnp.where(known, 0.0 if p < 9 else -1.0, ends)
        for rows in (slice(1, deep), slice(height - deep, height - 1)):
            ext[SELF + p, height + rows.start : height + rows.stop, 0:width] = ends[rows]

    wait_halo(recv_sem.at[BANDS], 0, band_rows, 0)
    by_displacement(height, 0, nrecv)
    wait_halo(recv_sem.at[CORNERS], 0, 0, corner_rows)
    unpack_starts(height, srecv.at[left], srecv.at[right])
    both = joined(tiles_of(crecv.at[left], stencil_tiles), tiles_of(crecv.at[right], stencil_tiles), deep)
    for p, (t, at) in enumerate(stencil_slots):
        value = roll(both[t], -at - deep, 1)
        if p < 9:
            ext[SELF + p, height:, width:] = value
        else:
            stencil[(p - 9) // 9, (p - 9) % 9, height:, width:] = value
    whole_cols, beyond = slice(None), slice(width, None)
    begin = [ext[START + r] for r in range(3)]
    begin_top = apply(begin, inside_rows, whole_cols)
    begin_corner = apply(begin, slice(height, None), beyond)

    def full(p):
        return ext[p]

    selfb = {(r, s): (lambda r=r, s=s: ext[SELF + 3 * r + s, 0:height, 0:width]) for r in range(3) for s in range(3)}
    nb = {
        (k, r, s): (lambda k=k, r=r, s=s: ext[NB + 9 * k + 3 * r + s, 0:height, 0:width])
        for k in range(edge_count) for r in range(3) for s in range(3)
    }
    elane = lax.broadcasted_iota(jnp.int32, (2 * height, 2 * width), 1)
    erow = lax.broadcasted_iota(jnp.int32, (2 * height, 2 * width), 0)

    last_row = jnp.where(me_n < narrow - 1, height + ITERS, height)
    back_row = jnp.where(me_n > 0, height + ITERS, 2 * height)
    last_lane = jnp.where(me_w < wide - 1, width + ITERS, width)
    back_lane = jnp.where(me_w > 0, 2 * width - ITERS, 2 * width)
    inside = jnp.logical_and(
        jnp.logical_or(erow < last_row, erow >= back_row), jnp.logical_or(elane < last_lane, elane >= back_lane)
    )
    far = jnp.logical_or(
        jnp.logical_and(erow > height, erow < height + deep),
        jnp.logical_and(erow > 2 * height - deep - 1, erow < 2 * height - 1),
    )
    far_known = jnp.logical_and(far, jnp.logical_and(elane > 1, elane < width - 2))
    inverse = [
        jnp.where(inside, 1.0 / jnp.where(far_known, 1.0, full(SELF + 4 * r)), 0.0) for r in range(3)
    ]
    diag = [selfb[r, r]() for r in range(3)]
    inv = [inverse[r][:height, :width] for r in range(3)]

    sent = jnp.logical_and(far, jnp.logical_and(elane > 0, elane < width - 1))
    spread = [
        jnp.concatenate([jnp.concatenate([firsts[r], firsts[r]], axis=0)] * 2, axis=1) for r in range(3)
    ]
    iterate = begin
    for number in range(ITERS):
        final = number == ITERS - 1
        rs, cs = (slice(0, height), slice(0, width)) if final else (slice(None), slice(None))
        if number == 0:
            outer = apply(begin, slice(height, None), inside_cols)
            applied = [
                jnp.concatenate([begin_top[r], jnp.concatenate([outer[r], begin_corner[r]], axis=1)], axis=0) for r in range(3)
            ]
        else:
            applied = apply(iterate, rs, cs)
        mine_it = [v[:height, :width] for v in iterate]
        mine_ap = [v[:height, :width] for v in applied]
        curvature = sum(mine_it[r] * mine_ap[r] for r in range(3))
        energy = sum(mine_it[r] * diag[r] * mine_it[r] for r in range(3))
        partial[number : number + 1] = jnp.sum(curvature, axis=0, keepdims=True)
        partial[number + 4 : number + 5] = jnp.sum(energy, axis=0, keepdims=True)
        iterate = [applied[r] * (inv[r] if final else inverse[r]) for r in range(3)]
        if number == 0:
            iterate = [jnp.where(sent, spread[r], iterate[r]) for r in range(3)]
        if number == 1:
            rest = [nrecv[0, 27 + r] + nrecv[1, 27 + r] for r in range(3)]
            iterate = [
                jnp.concatenate([
                    v[:height], jnp.concatenate([v[height:, :width] + rest[r], v[height:, width:]], axis=1),
                ], axis=0) for r, v in enumerate(iterate)
            ]

    totals = jnp.sum(partial[...], axis=1, keepdims=True)
    line = jnp.sum(jnp.where(lane == row, totals, 0.0), axis=0, keepdims=True)
    sumrow[...] = line
    allsum[me] = line
    to_all(sumrow, allsum.at[me], TOTALS)

    for r in range(3):
        iter_ref[r] = iterate[r]

    wait_halo(recv_sem.at[EDGES], *edge_rows)

    top, bottom = row == 0, row == height - 1
    lcol, rcol = htrecv[left], htrecv[right]
    corner_l = jnp.where(bottom, ctrecv[2 * left], ctrecv[2 * left + 1])
    corner_r = jnp.where(bottom, ctrecv[2 * right], ctrecv[2 * right + 1])
    for j in range(FIELDS):
        v = tent[j]
        w = jnp.where(bottom, vtrecv[0, j], vtrecv[1, j])
        vl = jnp.where(first, roll(lcol, -j, 1), roll(v, 1, 1))
        vr = jnp.where(last, roll(rcol, width - 1 - j, 1), roll(v, -1, 1))
        wl = jnp.where(first, roll(corner_l, -j, 1), roll(w, 1, 1))
        wr = jnp.where(last, roll(corner_r, width - 1 - j, 1), roll(w, -1, 1))
        pairs = ((vl, wl), (v, w), (vr, wr))
        up = [roll(jnp.where(bottom, b, a), 1, 0) for a, b in pairs]
        down = [roll(jnp.where(top, b, a), -1, 0) for a, b in pairs]
        for code, moved in enumerate(up + [vl, vr] + down):
            disp[j, code] = moved

    def piece(block, picked, index):
        unit, a0, a1, b0, b1, b2, g0, g1, g2 = picked
        for r in range(3):
            c0, c1, c2 = (block(r, s) * -inv[r] for s in range(3))
            out_ref[index, 0, r] = c0 * unit
            out_ref[index, 1, r] = c1 * unit
            out_ref[index, 2, r] = c2 * unit
            out_ref[index, 3, r] = c0 * a0 + c1 * a1
            out_ref[index, 4, r] = c0 * b0 + c1 * b1 + c2 * b2
            out_ref[index, 5, r] = c0 * g0 + c1 * g1 + c2 * g2

    piece(lambda r, s: selfb[r, s](), [fields[j] for j in range(FIELDS)], 0)
    for k in range(edge_count):
        masks = [nbr[k] == code for code in range(1, 8)]
        picked = []
        for j in range(FIELDS):
            value = disp[j, 0]
            for code in range(1, 8):
                value = jnp.where(masks[code - 1], disp[j, code], value)
            picked.append(value)
        piece(lambda r, s: nb[k, r, s](), picked, k + 1)

    loads[6].wait()
    some = gath.at[pl.ds(0, count - 1)]
    pltpu.make_async_copy(some, some, recv_sem.at[GATHER]).wait()
    across = width // TILE * wide
    tiles_x, tiles_y = width // TILE, height // TILE
    crow = lax.broadcasted_iota(jnp.int32, (share, width), 0)
    cgroup = lax.broadcasted_iota(jnp.int32, (share, width), 1) // TILE
    low, high = jnp.zeros((share, width), F32), jnp.zeros((share, width), F32)
    for j in range(share):
        wanted = cmap[me * share + j]
        tile_row, tile_col = wanted // across, lax.rem(wanted, across)
        slot = tile_col // tiles_x * narrow + tile_row // tiles_y
        lines = gath[slot]
        take = jnp.logical_and(crow == j, cgroup == lax.rem(tile_col, tiles_x))
        low = jnp.where(take, lines[0:1], low)
        high = jnp.where(take, lines[1:2], high)
    l00, mx, my, mz, l33, l43, l53, l44, l54, l55 = range(SUMS)
    entries = {
        (0, 0): (l00, 1), (1, 1): (l00, 1), (2, 2): (l00, 1),
        (3, 0): (my, -1), (3, 1): (mx, 1), (4, 1): (mz, -1), (4, 2): (my, 1), (5, 0): (mz, 1), (5, 2): (mx, -1),
        (3, 3): (l33, 1), (4, 3): (l43, 1), (5, 3): (l53, 1), (4, 4): (l44, 1), (5, 4): (l54, 1), (5, 5): (l55, 1),
    }
    outs = coarse_ref.shape[1]
    kind = lax.broadcasted_iota(jnp.int32, (1, outs), 1)
    chosen, sign = jnp.full((1, outs), -1, jnp.int32), jnp.zeros((1, outs), F32)
    for (n, m), (q, way) in entries.items():
        chosen = jnp.where(kind == 6 * m + n, q, chosen)
        sign = jnp.where(kind == 6 * m + n, float(way), sign)
    entry = lax.broadcasted_iota(jnp.int32, (width, outs), 0) % 8
    coarse = jnp.zeros(coarse_ref.shape, F32)
    for base, lines in ((0, low), (8, high)):
        pick = jnp.where(entry + base == chosen, sign, 0.0)
        coarse = coarse + jnp.dot(lines, pick, precision=lax.Precision.HIGHEST, preferred_element_type=F32)
    coarse_ref[...] = coarse

    wait_halo(
        send_sem, side_rows + edge_rows[0], end_rows + start_rows + band_rows + edge_rows[1], corner_rows + edge_rows[2],
        3 * (count - 1),
    )

    some = allsum.at[pl.ds(0, count - 1)]
    pltpu.make_async_copy(some, some, recv_sem.at[TOTALS]).wait()
    if count <= 64:
        lines = [allsum[d] for d in range(count)]
        while len(lines) > 1:
            lines = [a + b for a, b in zip(lines[::2], lines[1::2])] + ([lines[-1]] if len(lines) % 2 else [])
        total = lines[0]
    else:
        total = lax.fori_loop(0, count, lambda d, t: t + allsum[d], jnp.zeros((1, width), F32))
    values = [jnp.broadcast_to(total[:, i : i + 1], shape) for i in range(2 * ITERS)]
    ratios = [values[i + ITERS] / values[i] for i in range(ITERS)]
    growth = ratios[0]
    for i in range(1, ITERS):
        growth = growth * ratios[i]
    scale_ref[0] = ratios[ITERS - 1] * (4.0 / 3.0)
    scale_ref[1] = growth


def finish(raw, fields, iterate, scale, coarse, out_h, probe_h, coarse_h, out, probe, sem):
    weight = scale[0]
    base = {(0, 0): 0, (1, 1): 0, (2, 2): 0, (3, 0): 1, (3, 1): 2}
    for r in range(3):
        base[(4, r)] = 3 + r
        base[(5, r)] = 6 + r
    blocks, modes = raw.shape[:2]
    small = [pltpu.make_async_copy(coarse, coarse_h, sem.at[1]), pltpu.make_async_copy(probe, probe_h, sem.at[2])]
    small[0].start()
    for k in range(blocks):
        for m in range(modes):
            for r in range(3):
                value = raw[k, m, r] * weight
                out[k, m, r] = value + fields[base[(m, r)]] if k == 0 and (m, r) in base else value
        pltpu.make_async_copy(out.at[k], out_h.at[k], sem.at[0]).start()
    for r in range(3):
        probe[r] = iterate[r] * scale[1]
    small[1].start()
    for copy in small + [pltpu.make_async_copy(out, out_h, sem.at[0])]:
        copy.wait()


def local(wide, narrow, coords, member, start_vector, self_block, neighbour_block, neighbours, coarse_map):
    height, width = member.shape
    edge_count = neighbours.shape[0]
    count = wide * narrow
    share = coarse_map.shape[0] // count
    tile = (height, width)
    double = (2 * height, 2 * width)
    planes = 12 + 10 * edge_count
    tiles = edge_slots(planes - SELF, ITERS - 1, width)[1]
    stencil_tiles = edge_slots(STENCIL, ITERS - 1, width)[1]
    vmem = pltpu.VMEM
    dma = pltpu.SemaphoreType.DMA
    results = (
        jax.ShapeDtypeStruct((edge_count + 1, 6, 3) + tile, F32),
        jax.ShapeDtypeStruct((3,) + tile, F32),
        jax.ShapeDtypeStruct((share, 36), F32),
    )
    staged = pl.pallas_call(
        functools.partial(kernel, wide, narrow, share),
        out_shape=(
            results[0],
            jax.ShapeDtypeStruct((FIELDS,) + tile, F32),
            results[1],
            jax.ShapeDtypeStruct((2,) + tile, F32),
            results[2],
        ),
        in_specs=[pl.BlockSpec(memory_space=pl.ANY)] * 7,
        out_specs=(pl.BlockSpec(memory_space=pltpu.VMEM),) * 5,
        scratch_shapes=[
            vmem((3,) + tile, F32),
            vmem(tile, jnp.int32),
            vmem((edge_count,) + tile, jnp.int32),
            pltpu.SMEM(coarse_map.shape, jnp.int32),
            vmem((planes,) + double, F32),
            vmem((tiles + 1,) + tile, F32),
            vmem((8, 9) + double, F32),
            vmem((2,) + tile, F32),
            vmem((2, FIELDS, 1, width), F32),
            vmem((FIELDS, 8) + tile, F32),
            vmem((2, width), F32),
            vmem((count, 2, width), F32),
            vmem((1, width), F32),
            vmem((count, 1, width), F32),
            vmem((8, width), F32),
            vmem((stencil_tiles,) + tile, F32),
            vmem((2, tiles + 1) + tile, F32),
            vmem((tiles,) + tile, F32),
            vmem((2, stencil_tiles) + tile, F32),
            vmem((2,) + tile, F32),
            vmem((30,) + tile, F32),
            vmem((2, 30) + tile, F32),
            vmem((2,) + tile, F32),
            vmem((2, FIELDS, 1, width), F32),
            vmem((4, 1, width), F32),
            vmem((3,) + tile, F32),
            vmem((3,) + tile, F32),
            vmem((max((planes + 4) * height, 1024 + 3 * count), 1, width), F32),
            dma((2,)),
            dma(()),
            dma((7,)),
            pltpu.SemaphoreType.REGULAR((len(rounds_of(plane_width(wide), narrow)),)),
        ],
        compiler_params=pltpu.CompilerParams(collective_id=0, has_side_effects=True, vmem_limit_bytes=VMEM_LIMIT),
    )(*(
        pltpu.with_memory_space_constraint(value, pltpu.HBM)
        for value in (
            coords, member, start_vector, self_block.reshape((9,) + tile), neighbour_block.reshape((-1,) + tile),
            neighbours, coarse_map,
        )
    ))
    smoothed, probe, coarse = pl.pallas_call(
        finish,
        out_shape=results,
        in_specs=[pl.BlockSpec(memory_space=pltpu.VMEM)] * 5,
        out_specs=(pl.BlockSpec(memory_space=pl.ANY),) * 3,
        scratch_shapes=[
            vmem(results[0].shape, F32),
            vmem(results[1].shape, F32),
            dma((3,)),
        ],
        compiler_params=pltpu.CompilerParams(vmem_limit_bytes=VMEM_LIMIT),
    )(*staged)
    return smoothed, probe, coarse.T


def solution(mesh):
    return jax.shard_map(
        functools.partial(local, mesh.shape["wide"], mesh.shape["narrow"]),
        mesh=mesh,
        in_specs=(
            P(None, "narrow", "wide"),
            P("narrow", "wide"),
            P(None, "narrow", "wide"),
            P(None, None, "narrow", "wide"),
            P(None, None, None, "narrow", "wide"),
            P(None, "narrow", "wide"),
            P(),
        ),
        out_specs=(
            P(None, None, None, "narrow", "wide"),
            P(None, "narrow", "wide"),
            P(None, ("wide", "narrow")),
        ),
        check_vma=False,
    )
```

```python
import functools

import jax
import jax.numpy as jnp
from jax import lax
from jax.experimental import pallas as pl
from jax.experimental.pallas import tpu as pltpu
from jax.sharding import PartitionSpec as P

TILE = 8
ITERS = 4
MESH = pl.DeviceIdType.MESH
F32 = jnp.float32
SUMS = 10
FIELDS = 9
START, SELF, NB = 0, 3, 12
STENCIL = 81
STEPS = [(-1, -1), (-1, 0), (-1, 1), (0, -1), (0, 1), (1, -1), (1, 0), (1, 1)]
VMEM_LIMIT = 16 * 1024 * 1024


def roll(x, shift, axis):
    size = x.shape[axis]
    shift = shift % size
    return x if shift == 0 else pltpu.roll(x, shift, axis)


def plane_width(wide):
    best = max(size for size in range(1, wide + 1) if wide % size == 0 and size * size <= wide)
    return wide if best == 1 else best


def edge_slots(planes, columns, width):
    per = width // (2 * columns)
    return [(p // per, p % per * 2 * columns) for p in range(planes)], pl.cdiv(planes, per)


def rounds_of(across_plane, narrow):
    def doubled(size):
        steps = [1]
        while 2 * steps[-1] < size:
            steps.append(2 * steps[-1])
        return steps

    return [(0, 1)] + [(step, 0) for step in doubled(across_plane)] + [(0, step) for step in doubled(narrow)[1:]]


IN_NODES, IN_MAP = range(2)
SIDES, ENDS, CORNERS, BANDS, EDGES, GATHER, TOTALS = range(7)


def kernel(
    wide, narrow, share,
    coords_h, member_h, start_h, self_h, nb_h, nbr_h, cmap_h,
    out_ref, fields, iter_ref, scale_ref, coarse_ref,
    coords, member, nbr, cmap,
    ext, wpack, stencil, pack, tedges, disp, mine, gath, sumrow, allsum, partial,
    cpack, wrecv, erecv, crecv, srecv, htrecv, vtrecv, ctrecv, firsts_own, firsts,
    tally, in_sem, send_sem, recv_sem, round_sem,
):
    count = wide * narrow
    me_w, me_n = lax.axis_index("wide"), lax.axis_index("narrow")
    me = me_w * narrow + me_n
    barrier = pltpu.get_barrier_semaphore()
    across_plane = plane_width(wide)
    plane_count = wide // across_plane
    me_p, me_q = me_w // across_plane, lax.rem(me_w, across_plane)

    height, width = shape = member.shape
    edge_count = nbr.shape[0]
    codes_at = NB + 9 * edge_count
    planes = codes_at + edge_count
    deep = ITERS - 1
    start_slots, _ = edge_slots(SELF, ITERS, width)
    slots, tiles = edge_slots(planes - SELF, deep, width)
    stencil_slots, stencil_tiles = edge_slots(STENCIL, deep, width)
    rounds = rounds_of(across_plane, narrow)
    right, left = 0, 1

    def exists(code):
        dy, dx = STEPS[code]
        ok = None
        for step, at, size in ((dy, me_n, narrow), (dx, me_w, wide)):
            term = at > 0 if step < 0 else (at < size - 1 if step > 0 else None)
            if term is not None:
                ok = term if ok is None else jnp.logical_and(ok, term)
        return ok

    present_at = [exists(code) for code in range(8)]

    def target(code):
        dy, dx = STEPS[code]
        return (me_w + dx, me_n + dy)

    def greet(cond, device):
        @pl.when(cond)
        def _():
            pl.semaphore_signal(barrier, inc=1, device_id=device, device_id_type=MESH)
        return cond.astype(jnp.int32)

    expected = 0
    for code in (1, 6):
        expected = expected + greet(present_at[code], target(code))

    def own(first, size):
        return ext.at[first : first + size, 0:height, 0:width]

    loads = [
        pltpu.make_async_copy(src, dst, in_sem.at[i])
        for src, dst, i in (
            (nb_h, own(NB, nb_h.shape[0]), IN_NODES), (self_h, own(SELF, 9), IN_NODES), (start_h, own(START, 3), IN_NODES),
            (nbr_h, nbr, IN_NODES), (coords_h, coords, IN_NODES), (member_h, member, IN_NODES), (cmap_h, cmap, IN_MAP),
        )
    ]
    for load in loads:
        load.start()

    def wait_rows(sem, rows):
        some = tally.at[0:rows]
        pltpu.make_async_copy(some, some, sem).wait()

    sides_here = (me_w > 0).astype(jnp.int32) + (me_w < wide - 1).astype(jnp.int32)
    ends_here = (me_n > 0).astype(jnp.int32) + (me_n < narrow - 1).astype(jnp.int32)

    def wait_halo(sem, side, end, corner, more=0):
        for a in range(min(wide - 1, 1), min(wide - 1, 2) + 1):
            for b in range(min(narrow - 1, 1), min(narrow - 1, 2) + 1):
                rows = a * side + b * end + a * b * corner + more
                if rows:
                    pl.when(jnp.logical_and(sides_here == a, ends_here == b))(functools.partial(wait_rows, sem, rows))

    for code in (3, 4):
        expected = expected + greet(present_at[code], target(code))

    for p in range(plane_count):
        w = p * across_plane + me_q
        expected = expected + greet(jnp.abs(w - me_w) > 1, (w, me_n))

    def partners(number):
        for way in (-1, 1):
            dq, dn = (way * step for step in rounds[number])
            q, n = me_q + dq, me_n + dn
            yield jnp.logical_and(jnp.logical_and(q >= 0, q < across_plane), jnp.logical_and(n >= 0, n < narrow)), (me_w + dq, n)

    def tell(number):
        for cond, device in partners(number):
            @pl.when(cond)
            def _(device=device):
                pl.semaphore_signal(round_sem.at[number], inc=1, device_id=device, device_id_type=MESH)

    def hear(number):
        pl.semaphore_wait(round_sem.at[number], sum(cond.astype(jnp.int32) for cond, _ in partners(number)))

    def corner_refs(operator, start, low):
        at = 0 if low else height - deep
        start_at = 0 if low else height - ITERS
        return [operator.at[:, at : at + deep, :], start.at[start_at : start_at + ITERS, :]]

    for code in range(8):
        dy, dx = STEPS[code]
        @pl.when(jnp.logical_not(present_at[code]))
        def _(code=code, dy=dy, dx=dx):
            side = right if dx > 0 else left
            if dx == 0:
                at = height if dy > 0 else height + ITERS
                ext[:, at : at + ITERS, 0:width] = jnp.zeros((planes, ITERS, width), F32)
                vtrecv[0 if dy < 0 else 1] = jnp.zeros(vtrecv.shape[1:], F32)
                at = deep - 1 if dy > 0 else height - deep
                firsts[:, at : at + 1, :] = jnp.zeros((3, 1, width), F32)
                erecv[:, at : at + 1, :] = jnp.zeros((tiles, 1, width), F32)
            elif dy == 0:
                wrecv[side] = jnp.zeros(wrecv.shape[1:], F32)
                htrecv[side] = jnp.zeros(htrecv.shape[1:], F32)
            else:
                for ref in corner_refs(crecv.at[side], srecv.at[side], dy > 0):
                    ref[...] = jnp.zeros(ref.shape, F32)
                ctrecv[2 * side + (0 if dy < 0 else 1)] = jnp.zeros(ctrecv.shape[1:], F32)

    lane = lax.broadcasted_iota(jnp.int32, shape, 1)
    row = lax.broadcasted_iota(jnp.int32, shape, 0)
    first, last = lane == 0, lane == width - 1

    pl.semaphore_wait(barrier, expected)
    tell(0)
    wait_rows(in_sem.at[IN_NODES], (planes + 4) * height)
    for k in range(edge_count):
        ext[codes_at + k, 0:height, 0:width] = nbr[k].astype(F32)

    def send(code, pairs, group):
        made = [
            pltpu.make_async_remote_copy(
                src_ref=src, dst_ref=dst, send_sem=send_sem, recv_sem=recv_sem.at[group],
                device_id=target(code), device_id_type=MESH,
            )
            for src, dst in pairs
        ]

        @pl.when(present_at[code])
        def _():
            for copy in made:
                copy.start()

    bands = ((START, 3, ITERS), (SELF, 9, deep - 1), (NB, 9 * (edge_count - 1), deep - 1), (codes_at - 9, 9 + edge_count, deep - 1))

    def band_pairs(code, band):
        base, size, rows = band
        here, there = (0, height) if STEPS[code][0] < 0 else (height - rows, height + 2 * ITERS - rows)
        return [(
            ext.at[base : base + size, here : here + rows, 0:width],
            ext.at[base : base + size, there : there + rows, 0:width],
        )]

    def end_pairs(code):
        here = deep - 1 if STEPS[code][0] < 0 else height - deep
        return [(wpack.at[0:tiles, here : here + 1, :], erecv.at[:, here : here + 1, :])]

    def first_pairs(code):
        here = deep - 1 if STEPS[code][0] < 0 else height - deep
        return [(firsts_own.at[:, here : here + 1, :], firsts.at[:, here : here + 1, :])]

    for code in (1, 6):
        send(code, band_pairs(code, bands[0]), ENDS)
        send(code, band_pairs(code, bands[1]), BANDS)
    def packed(sources, slots, columns):
        result = []
        for source, (t, at) in zip(sources, slots):
            moved = roll(source(), at + columns, 1)
            if at == 0:
                result.append(moved)
            else:
                result[t] = jnp.where(lane >= at, moved, result[t])
        return result

    def main(p):
        return lambda: ext[p, 0:height, 0:width]

    raw = packed([main(SELF + p) for p in range(planes - SELF)], slots, deep)
    starts = packed([main(START + r) for r in range(SELF)], start_slots, ITERS)
    for t, value in enumerate(raw + starts):
        wpack[t] = value

    for code in (1, 6):
        send(code, end_pairs(code), ENDS)
        send(code, band_pairs(code, bands[2]) + band_pairs(code, bands[3]), BANDS)
    for code in (3, 4):
        send(code, [(wpack, wrecv.at[left if code == 4 else right])], SIDES)

    def by_displacement(r0, c0):
        def at(p):
            return ext[p, r0 : r0 + height, c0 : c0 + width]

        for group in range(0, 8, 2):
            masks = {(code, k): at(codes_at + k) == code for code in (group, group + 1) for k in range(edge_count)}
            for q in range(9):
                blocks = [at(NB + 9 * k + q) for k in range(edge_count)]
                for code in (group, group + 1):
                    value = jnp.zeros(shape, F32)
                    for k in range(edge_count):
                        value = jnp.where(masks[code, k], blocks[k], value)
                    stencil[code, q, r0 : r0 + height, c0 : c0 + width] = value

    def apply(iterate, rs, cs):
        applied = [sum(ext[SELF + 3 * r + s, rs, cs] * iterate[s][rs, cs] for s in range(3)) for r in range(3)]
        for s in range(3):
            for dx in (0, -1, 1):
                shifted = roll(iterate[s], -dx, 1)
                for dy in (-1, 0, 1):
                    if (dy, dx) == (0, 0):
                        continue
                    code = STEPS.index((dy, dx))
                    moved = roll(shifted, -dy, 0)[rs, cs]
                    for r in range(3):
                        applied[r] = applied[r] + stencil[code, 3 * r + s, rs, cs] * moved
        return applied

    by_displacement(0, 0)
    shifted_main = [main(SELF + q) for q in range(9)] + [
        lambda code=code, q=q: stencil[code, q, 0:height, 0:width] for code in range(8) for q in range(9)
    ]
    for t, value in enumerate(packed(shifted_main, stencil_slots, deep)):
        cpack[t] = value
    inside_rows, inside_cols = slice(0, height), slice(0, width)
    applied = apply([ext[START + r, 0:height, 0:width] for r in range(3)], inside_rows, inside_cols)
    for r in range(3):
        firsts_own[r] = applied[r] * (1.0 / ext[SELF + 4 * r, 0:height, 0:width])
    for code in (1, 6):
        send(code, first_pairs(code), BANDS)
    hear(0)
    tell(1)
    for code in (0, 2, 5, 7):
        dy, dx = STEPS[code]
        side = right if dx < 0 else left
        send(code, list(zip(
            corner_refs(cpack, wpack.at[tiles], dy < 0), corner_refs(crecv.at[side], srecv.at[side], dy < 0),
        )), CORNERS)

    present = member[...].astype(F32)
    x, y, z = (coords[r] * present for r in range(3))
    products = [present * present, x * present, y * present, z * present, x * x, y * y, z * z, x * y, x * z, y * z]
    sum_tiles = []
    for base in (0, 8):
        tile = jnp.zeros(shape, F32)
        for q, product in enumerate(products[base : base + 8]):
            tile = jnp.where(row == q, jnp.sum(product, axis=0, keepdims=True), tile)
        for s in (1, 2, 4):
            tile = tile + jnp.where((lane & s) != 0, roll(tile, s, 1), roll(tile, -s, 1))
        sum_tiles.append(tile)
    sums = [sum_tiles[q // 8][q % 8 : q % 8 + 1, :] for q in range(SUMS)]

    def factor(sums):
        n, sx, sy, sz, xx, yy, zz, xy, xz, yz = sums
        l00 = jnp.sqrt(n)
        mx, my, mz = sx / l00, sy / l00, sz / l00
        l33 = jnp.sqrt(xx + yy - mx * mx - my * my)
        l43 = (mx * mz - xz) / l33
        l53 = (my * mz - yz) / l33
        l44 = jnp.sqrt(yy + zz - my * my - mz * mz - l43 * l43)
        l54 = (mx * my - xy - l53 * l43) / l44
        l55 = jnp.sqrt(xx + zz - mx * mx - mz * mz - l53 * l53 - l54 * l54)
        return l00, mx, my, mz, l33, l43, l53, l44, l54, l55

    parts = factor(sums)
    l00, mx, my, mz, l33, l43, l53, l44, l54, l55 = parts
    unit = present / l00
    cx, cy, cz = x - mx * unit, y - my * unit, z - mz * unit
    a0, a1 = -cy / l33, cx / l33
    b0, b1, b2 = -l43 * a0 / l44, (-cz - l43 * a1) / l44, cy / l44
    g0 = (cz - l53 * a0 - l54 * b0) / l55
    g1 = (-l53 * a1 - l54 * b1) / l55
    g2 = (-cx - l54 * b2) / l55
    tent = [unit, a0, a1, b0, b1, b2, g0, g1, g2]
    packl, packr = jnp.zeros(shape, F32), jnp.zeros(shape, F32)
    for j, field in enumerate(tent):
        fields[j] = field
        packl = jnp.where(lane == j, roll(field, j, 1), packl)
        packr = jnp.where(lane == j, roll(field, j + 1, 1), packr)
        tedges[0, j] = field[:1]
        tedges[1, j] = field[height - 1 :]
    pack[left] = packl
    pack[right] = packr
    lane_row = lax.broadcasted_iota(jnp.int32, (1, width), 1) % 8
    rows_out = []
    for base in (0, 8):
        line = jnp.zeros((1, width), F32)
        for q, part in enumerate(parts[base : base + 8]):
            line = jnp.where(lane_row == q, part, line)
        rows_out.append(line)
    mine[0:1] = rows_out[0]
    mine[1:2] = rows_out[1]
    gath[me] = jnp.concatenate(rows_out, axis=0)

    for code in range(8):
        dy, dx = STEPS[code]
        mine_side, their_side = (left, right) if dx < 0 else (right, left)
        if dx == 0:
            src, dst = tedges.at[0 if dy < 0 else 1], vtrecv.at[1 if dy < 0 else 0]
        elif dy == 0:
            src, dst = pack.at[mine_side], htrecv.at[their_side]
        else:
            edge = 0 if dy < 0 else height - 1
            src = pack.at[mine_side, edge : edge + 1, :]
            dst = ctrecv.at[2 * their_side + (1 if dy < 0 else 0)]
        send(code, [(src, dst)], EDGES)

    for number in range(1, len(rounds) - 1):
        hear(number)
        tell(number + 1)
    if len(rounds) > 1:
        hear(len(rounds) - 1)

    def to_all(src, dst, group):
        def one(i):
            k = i // narrow
            w = jnp.where(2 * me_w < wide, wide - 1 - k, k)
            n = lax.rem(me_n + 1 + i, narrow)

            @pl.when(jnp.logical_or(w != me_w, n != me_n))
            def _():
                pltpu.make_async_remote_copy(
                    src_ref=src, dst_ref=dst, send_sem=send_sem, recv_sem=recv_sem.at[group],
                    device_id=(w, n), device_id_type=MESH,
                ).start()

        if count <= 64:
            for i in range(count):
                one(i)
        else:
            pl.loop(0, count)(one)

    to_all(mine, gath.at[me], GATHER)

    def joined(from_left, from_right, columns):
        takes_left = lax.rem(lane, 2 * columns) < columns
        return [jnp.where(takes_left, a[...], b[...]) for a, b in zip(from_left, from_right)]

    def tiles_of(ref, count_of):
        return [ref.at[t] for t in range(count_of)]

    def unpack_starts(r0, from_left, from_right):
        both, = joined([from_left], [from_right], ITERS)
        for r, (_, at) in enumerate(start_slots):
            ext[START + r, r0 : r0 + height, width:] = roll(both, -at - ITERS, 1)

    side_rows, start_rows = (tiles + 1) * height, SELF * ITERS
    corner_rows, end_rows = stencil_tiles * deep + ITERS, tiles
    band_rows = (planes - SELF) * (deep - 1) + 3
    edge_rows = (height, FIELDS, 1)
    wait_halo(recv_sem.at[SIDES], side_rows, 0, 0)
    unpack_starts(0, wrecv.at[left, tiles], wrecv.at[right, tiles])
    both = joined(tiles_of(wrecv.at[left], tiles), tiles_of(wrecv.at[right], tiles), deep)
    for p, (t, at) in enumerate(slots):
        ext[SELF + p, 0:height, width:] = roll(both[t], -at - deep, 1)
    by_displacement(0, width)
    wait_halo(recv_sem.at[ENDS], 0, end_rows + start_rows, 0)
    for p, (t, at) in enumerate(slots):
        ends = roll(erecv[t], -at - deep, 1)
        ext[SELF + p, height + deep - 1 : height + deep, 0:width] = ends[deep - 1 : deep]
        ext[SELF + p, 2 * height - deep : 2 * height - deep + 1, 0:width] = ends[height - deep : height - deep + 1]

    wait_halo(recv_sem.at[CORNERS], 0, 0, corner_rows)
    unpack_starts(height, srecv.at[left], srecv.at[right])
    both = joined(tiles_of(crecv.at[left], stencil_tiles), tiles_of(crecv.at[right], stencil_tiles), deep)
    for p, (t, at) in enumerate(stencil_slots):
        value = roll(both[t], -at - deep, 1)
        if p < 9:
            ext[SELF + p, height:, width:] = value
        else:
            stencil[(p - 9) // 9, (p - 9) % 9, height:, width:] = value
    whole_cols, beyond = slice(None), slice(width, None)
    begin = [ext[START + r] for r in range(3)]
    begin_top = apply(begin, inside_rows, whole_cols)
    begin_corner = apply(begin, slice(height, None), beyond)
    wait_halo(recv_sem.at[BANDS], 0, band_rows, 0)
    by_displacement(height, 0)

    def full(p):
        return ext[p]

    selfb = {(r, s): (lambda r=r, s=s: ext[SELF + 3 * r + s, 0:height, 0:width]) for r in range(3) for s in range(3)}
    nb = {
        (k, r, s): (lambda k=k, r=r, s=s: ext[NB + 9 * k + 3 * r + s, 0:height, 0:width])
        for k in range(edge_count) for r in range(3) for s in range(3)
    }
    elane = lax.broadcasted_iota(jnp.int32, (2 * height, 2 * width), 1)
    erow = lax.broadcasted_iota(jnp.int32, (2 * height, 2 * width), 0)

    last_row = jnp.where(me_n < narrow - 1, height + ITERS, height)
    back_row = jnp.where(me_n > 0, height + ITERS, 2 * height)
    last_lane = jnp.where(me_w < wide - 1, width + ITERS, width)
    back_lane = jnp.where(me_w > 0, 2 * width - ITERS, 2 * width)
    inside = jnp.logical_and(
        jnp.logical_or(erow < last_row, erow >= back_row), jnp.logical_or(elane < last_lane, elane >= back_lane)
    )
    inverse = [jnp.where(inside, 1.0 / full(SELF + 4 * r), 0.0) for r in range(3)]
    diag = [selfb[r, r]() for r in range(3)]
    inv = [inverse[r][:height, :width] for r in range(3)]

    sent = jnp.logical_and(
        jnp.logical_or(erow == height + deep - 1, erow == 2 * height - deep),
        jnp.logical_and(elane > 0, elane < width - 1),
    )
    spread = [
        jnp.concatenate([jnp.concatenate([firsts[r], firsts[r]], axis=0)] * 2, axis=1) for r in range(3)
    ]
    iterate = begin
    for number in range(ITERS):
        final = number == ITERS - 1
        rs, cs = (slice(0, height), slice(0, width)) if final else (slice(None), slice(None))
        if number == 0:
            outer = apply(begin, slice(height, None), inside_cols)
            applied = [
                jnp.concatenate([begin_top[r], jnp.concatenate([outer[r], begin_corner[r]], axis=1)], axis=0) for r in range(3)
            ]
        else:
            applied = apply(iterate, rs, cs)
        mine_it = [v[:height, :width] for v in iterate]
        mine_ap = [v[:height, :width] for v in applied]
        curvature = sum(mine_it[r] * mine_ap[r] for r in range(3))
        energy = sum(mine_it[r] * diag[r] * mine_it[r] for r in range(3))
        partial[number : number + 1] = jnp.sum(curvature, axis=0, keepdims=True)
        partial[number + 4 : number + 5] = jnp.sum(energy, axis=0, keepdims=True)
        iterate = [applied[r] * (inv[r] if final else inverse[r]) for r in range(3)]
        if number == 0:
            iterate = [jnp.where(sent, spread[r], iterate[r]) for r in range(3)]

    totals = jnp.sum(partial[...], axis=1, keepdims=True)
    line = jnp.sum(jnp.where(lane == row, totals, 0.0), axis=0, keepdims=True)
    sumrow[...] = line
    allsum[me] = line
    to_all(sumrow, allsum.at[me], TOTALS)

    for r in range(3):
        iter_ref[r] = iterate[r]

    wait_halo(recv_sem.at[EDGES], *edge_rows)

    top, bottom = row == 0, row == height - 1
    lcol, rcol = htrecv[left], htrecv[right]
    corner_l = jnp.where(bottom, ctrecv[2 * left], ctrecv[2 * left + 1])
    corner_r = jnp.where(bottom, ctrecv[2 * right], ctrecv[2 * right + 1])
    for j in range(FIELDS):
        v = tent[j]
        w = jnp.where(bottom, vtrecv[0, j], vtrecv[1, j])
        vl = jnp.where(first, roll(lcol, -j, 1), roll(v, 1, 1))
        vr = jnp.where(last, roll(rcol, width - 1 - j, 1), roll(v, -1, 1))
        wl = jnp.where(first, roll(corner_l, -j, 1), roll(w, 1, 1))
        wr = jnp.where(last, roll(corner_r, width - 1 - j, 1), roll(w, -1, 1))
        pairs = ((vl, wl), (v, w), (vr, wr))
        up = [roll(jnp.where(bottom, b, a), 1, 0) for a, b in pairs]
        down = [roll(jnp.where(top, b, a), -1, 0) for a, b in pairs]
        for code, moved in enumerate(up + [vl, vr] + down):
            disp[j, code] = moved

    def piece(block, picked, index):
        unit, a0, a1, b0, b1, b2, g0, g1, g2 = picked
        for r in range(3):
            c0, c1, c2 = (block(r, s) * -inv[r] for s in range(3))
            out_ref[index, 0, r] = c0 * unit
            out_ref[index, 1, r] = c1 * unit
            out_ref[index, 2, r] = c2 * unit
            out_ref[index, 3, r] = c0 * a0 + c1 * a1
            out_ref[index, 4, r] = c0 * b0 + c1 * b1 + c2 * b2
            out_ref[index, 5, r] = c0 * g0 + c1 * g1 + c2 * g2

    piece(lambda r, s: selfb[r, s](), [fields[j] for j in range(FIELDS)], 0)
    for k in range(edge_count):
        masks = [nbr[k] == code for code in range(1, 8)]
        picked = []
        for j in range(FIELDS):
            value = disp[j, 0]
            for code in range(1, 8):
                value = jnp.where(masks[code - 1], disp[j, code], value)
            picked.append(value)
        piece(lambda r, s: nb[k, r, s](), picked, k + 1)

    loads[6].wait()
    some = gath.at[pl.ds(0, count - 1)]
    pltpu.make_async_copy(some, some, recv_sem.at[GATHER]).wait()
    across = width // TILE * wide
    tiles_x, tiles_y = width // TILE, height // TILE
    crow = lax.broadcasted_iota(jnp.int32, (share, width), 0)
    cgroup = lax.broadcasted_iota(jnp.int32, (share, width), 1) // TILE
    low, high = jnp.zeros((share, width), F32), jnp.zeros((share, width), F32)
    for j in range(share):
        wanted = cmap[me * share + j]
        tile_row, tile_col = wanted // across, lax.rem(wanted, across)
        slot = tile_col // tiles_x * narrow + tile_row // tiles_y
        lines = gath[slot]
        take = jnp.logical_and(crow == j, cgroup == lax.rem(tile_col, tiles_x))
        low = jnp.where(take, lines[0:1], low)
        high = jnp.where(take, lines[1:2], high)
    l00, mx, my, mz, l33, l43, l53, l44, l54, l55 = range(SUMS)
    entries = {
        (0, 0): (l00, 1), (1, 1): (l00, 1), (2, 2): (l00, 1),
        (3, 0): (my, -1), (3, 1): (mx, 1), (4, 1): (mz, -1), (4, 2): (my, 1), (5, 0): (mz, 1), (5, 2): (mx, -1),
        (3, 3): (l33, 1), (4, 3): (l43, 1), (5, 3): (l53, 1), (4, 4): (l44, 1), (5, 4): (l54, 1), (5, 5): (l55, 1),
    }
    outs = coarse_ref.shape[1]
    kind = lax.broadcasted_iota(jnp.int32, (1, outs), 1)
    chosen, sign = jnp.full((1, outs), -1, jnp.int32), jnp.zeros((1, outs), F32)
    for (n, m), (q, way) in entries.items():
        chosen = jnp.where(kind == 6 * m + n, q, chosen)
        sign = jnp.where(kind == 6 * m + n, float(way), sign)
    entry = lax.broadcasted_iota(jnp.int32, (width, outs), 0) % 8
    coarse = jnp.zeros(coarse_ref.shape, F32)
    for base, lines in ((0, low), (8, high)):
        pick = jnp.where(entry + base == chosen, sign, 0.0)
        coarse = coarse + jnp.dot(lines, pick, precision=lax.Precision.HIGHEST, preferred_element_type=F32)
    coarse_ref[...] = coarse

    wait_halo(
        send_sem, side_rows + edge_rows[0], end_rows + start_rows + band_rows + edge_rows[1], corner_rows + edge_rows[2],
        3 * (count - 1),
    )

    some = allsum.at[pl.ds(0, count - 1)]
    pltpu.make_async_copy(some, some, recv_sem.at[TOTALS]).wait()
    if count <= 64:
        lines = [allsum[d] for d in range(count)]
        while len(lines) > 1:
            lines = [a + b for a, b in zip(lines[::2], lines[1::2])] + ([lines[-1]] if len(lines) % 2 else [])
        total = lines[0]
    else:
        total = lax.fori_loop(0, count, lambda d, t: t + allsum[d], jnp.zeros((1, width), F32))
    values = [jnp.broadcast_to(total[:, i : i + 1], shape) for i in range(2 * ITERS)]
    ratios = [values[i + ITERS] / values[i] for i in range(ITERS)]
    growth = ratios[0]
    for i in range(1, ITERS):
        growth = growth * ratios[i]
    scale_ref[0] = ratios[ITERS - 1] * (4.0 / 3.0)
    scale_ref[1] = growth


def finish(raw, fields, iterate, scale, coarse, out_h, probe_h, coarse_h, out, probe, sem):
    weight = scale[0]
    base = {(0, 0): 0, (1, 1): 0, (2, 2): 0, (3, 0): 1, (3, 1): 2}
    for r in range(3):
        base[(4, r)] = 3 + r
        base[(5, r)] = 6 + r
    blocks, modes = raw.shape[:2]
    small = [pltpu.make_async_copy(coarse, coarse_h, sem.at[1]), pltpu.make_async_copy(probe, probe_h, sem.at[2])]
    small[0].start()
    for k in range(blocks):
        for m in range(modes):
            for r in range(3):
                value = raw[k, m, r] * weight
                out[k, m, r] = value + fields[base[(m, r)]] if k == 0 and (m, r) in base else value
        pltpu.make_async_copy(out.at[k], out_h.at[k], sem.at[0]).start()
    for r in range(3):
        probe[r] = iterate[r] * scale[1]
    small[1].start()
    for copy in small + [pltpu.make_async_copy(out, out_h, sem.at[0])]:
        copy.wait()


def local(wide, narrow, coords, member, start_vector, self_block, neighbour_block, neighbours, coarse_map):
    height, width = member.shape
    edge_count = neighbours.shape[0]
    count = wide * narrow
    share = coarse_map.shape[0] // count
    tile = (height, width)
    double = (2 * height, 2 * width)
    planes = 12 + 10 * edge_count
    tiles = edge_slots(planes - SELF, ITERS - 1, width)[1]
    stencil_tiles = edge_slots(STENCIL, ITERS - 1, width)[1]
    vmem = pltpu.VMEM
    dma = pltpu.SemaphoreType.DMA
    results = (
        jax.ShapeDtypeStruct((edge_count + 1, 6, 3) + tile, F32),
        jax.ShapeDtypeStruct((3,) + tile, F32),
        jax.ShapeDtypeStruct((share, 36), F32),
    )
    staged = pl.pallas_call(
        functools.partial(kernel, wide, narrow, share),
        out_shape=(
            results[0],
            jax.ShapeDtypeStruct((FIELDS,) + tile, F32),
            results[1],
            jax.ShapeDtypeStruct((2,) + tile, F32),
            results[2],
        ),
        in_specs=[pl.BlockSpec(memory_space=pl.ANY)] * 7,
        out_specs=(pl.BlockSpec(memory_space=pltpu.VMEM),) * 5,
        scratch_shapes=[
            vmem((3,) + tile, F32),
            vmem(tile, jnp.int32),
            vmem((edge_count,) + tile, jnp.int32),
            pltpu.SMEM(coarse_map.shape, jnp.int32),
            vmem((planes,) + double, F32),
            vmem((tiles + 1,) + tile, F32),
            vmem((8, 9) + double, F32),
            vmem((2,) + tile, F32),
            vmem((2, FIELDS, 1, width), F32),
            vmem((FIELDS, 8) + tile, F32),
            vmem((2, width), F32),
            vmem((count, 2, width), F32),
            vmem((1, width), F32),
            vmem((count, 1, width), F32),
            vmem((8, width), F32),
            vmem((stencil_tiles,) + tile, F32),
            vmem((2, tiles + 1) + tile, F32),
            vmem((tiles,) + tile, F32),
            vmem((2, stencil_tiles) + tile, F32),
            vmem((2,) + tile, F32),
            vmem((2,) + tile, F32),
            vmem((2, FIELDS, 1, width), F32),
            vmem((4, 1, width), F32),
            vmem((3,) + tile, F32),
            vmem((3,) + tile, F32),
            vmem((max((planes + 4) * height, 1024 + 3 * count), 1, width), F32),
            dma((2,)),
            dma(()),
            dma((7,)),
            pltpu.SemaphoreType.REGULAR((len(rounds_of(plane_width(wide), narrow)),)),
        ],
        compiler_params=pltpu.CompilerParams(collective_id=0, has_side_effects=True, vmem_limit_bytes=VMEM_LIMIT),
    )(*(
        pltpu.with_memory_space_constraint(value, pltpu.HBM)
        for value in (
            coords, member, start_vector, self_block.reshape((9,) + tile), neighbour_block.reshape((-1,) + tile),
            neighbours, coarse_map,
        )
    ))
    smoothed, probe, coarse = pl.pallas_call(
        finish,
        out_shape=results,
        in_specs=[pl.BlockSpec(memory_space=pltpu.VMEM)] * 5,
        out_specs=(pl.BlockSpec(memory_space=pl.ANY),) * 3,
        scratch_shapes=[
            vmem(results[0].shape, F32),
            vmem(results[1].shape, F32),
            dma((3,)),
        ],
        compiler_params=pltpu.CompilerParams(vmem_limit_bytes=VMEM_LIMIT),
    )(*staged)
    return smoothed, probe, coarse.T


def solution(mesh):
    return jax.shard_map(
        functools.partial(local, mesh.shape["wide"], mesh.shape["narrow"]),
        mesh=mesh,
        in_specs=(
            P(None, "narrow", "wide"),
            P("narrow", "wide"),
            P(None, "narrow", "wide"),
            P(None, None, "narrow", "wide"),
            P(None, None, None, "narrow", "wide"),
            P(None, "narrow", "wide"),
            P(),
        ),
        out_specs=(
            P(None, None, None, "narrow", "wide"),
            P(None, "narrow", "wide"),
            P(None, ("wide", "narrow")),
        ),
        check_vma=False,
    )
```
